256 devices in a mesh: gx: 8 (over x, y_hi), gy: 4 (over y_lo, core), gz: 8 (over z).
Axes of the slice: x: 4, y: 4 (y_hi: 2, y_lo: 2; y = y_hi * 2 + y_lo), z: 8, core: 2. Of those that a mesh axis runs over, the one named last changes fastest.
Arguments:
- density: float32 [40, 20, 1280], P('gx', 'gy', 'gz'), may hold values from 0.5 to 2
- velocity: float32 [3, 40, 20, 1280], P(None, 'gx', 'gy', 'gz'), may hold values from -3.2 to 3.2
- pressure: float32 [40, 20, 1280], P('gx', 'gy', 'gz'), may hold values from 0.5 to 2
- blending: float32 [8, 4, 256], P('gx', 'gy', 'gz'), may hold values from 0 to 0.6
- face_signal_weights: bfloat16 [4, 10240, 4096], P(None, ('gx', 'gy'), 'gz'), may hold values from -0.013671875 to 0.013671875
- surf_id: int32 [30720], P(('gx', 'gy', 'gz')), may hold values from -1 to 10239, as said below
- surface_face_code: int32 [30720], P(('gx', 'gy', 'gz')), may hold values from 0 to 191, as said below
Outputs:
- tendency: float32 [5, 40, 20, 1280], P(None, 'gx', 'gy', 'gz')
- signals: float32 [4096], P(('gz', 'gx', 'gy'))
The draws below stay inside these ranges and needn't reach their ends.
Inputs may be any that keep to these rules, and one draw needn't show every extreme that they name: `surf_id`: every face id 0 to 10239 stands in exactly one slot; a device's listed faces fill its first slots and its other slots hold -1. A quarter of the devices list exactly 120 faces, the others at most 40. `surface_face_code`: the codes of one device are distinct.
All inputs are finite; a program needn't handle non-finite values.
Results may differ from the reference program's by a relative error of at most 0.0029.
Values may be sent and summed in bfloat16 or wider, within the bound.
No kernel may reach another device: no remote copies, remote signals or barrier semaphores. Data moves between devices by JAX's collectives and lax.ppermute only.
A program may use at most 128 MiB of HBM per device.

```python
import math
import jax
import jax.numpy as jnp
import numpy as np
from jax import lax

QN = 4
EX = 1
EY = 1
EZ = 32
FACE_DEV = 40
ALL_DEVICES = 256
ELEMS = 32
SLOTS = 120
FACES = 10240
SIG = 4096
ELEMENTS_FIRST = 8
ELEMENTS_SECOND = 4
ELEMENTS_THIRD = 256
NX = 40
NY = 20
NZ = 1280
N_GX = 8
N_GY = 4
N_GZ = 8


def face_counts(key):
    group_total = ALL_DEVICES // 4
    device_order = jax.random.permutation(jax.random.fold_in(key, 1), ALL_DEVICES).astype(jnp.int32)
    second = jax.random.randint(jax.random.fold_in(key, 2), (group_total,), 0, FACE_DEV + 1, dtype=jnp.int32)
    third = jax.random.randint(jax.random.fold_in(key, 3), (group_total,), 0, FACE_DEV + 1, dtype=jnp.int32) % (FACE_DEV - second + 1)
    fourth = FACE_DEV - second - third
    busiest = jnp.full((group_total,), SLOTS, dtype=jnp.int32)
    in_order = jnp.stack([busiest, second, third, fourth], axis=1).reshape(-1)
    return jnp.zeros((ALL_DEVICES,), jnp.int32).at[device_order].set(in_order)


def draw_surf_id(key, part):
    counts = face_counts(jax.random.fold_in(key, 101))
    offsets = jnp.cumsum(counts) - counts
    shuffled = jax.random.permutation(jax.random.fold_in(key, 102), FACES).astype(jnp.int32)
    slot_index = jnp.arange(SLOTS, dtype=jnp.int32)
    occupied = slot_index[None, :] < counts[:, None]
    position = jnp.clip(offsets[:, None] + slot_index[None, :], 0, FACES - 1)
    return jnp.where(occupied, shuffled[position], -1).reshape(-1).astype(jnp.int32)


def draw_surface_face_code(key, part):
    device_keys = jax.random.split(jax.random.fold_in(key, 201), ALL_DEVICES)

    def one_device(device_key):
        return jax.random.permutation(device_key, 6 * ELEMS)[:SLOTS]
    return jax.vmap(one_device)(device_keys).reshape(-1).astype(jnp.int32)


def raised(entries, stream_key, source, target, shards_of, factor):
    def block_of(axis_at):
        return (jnp.arange(entries.shape[axis_at]) // (entries.shape[axis_at] // shards_of)).reshape((-1,) + (1,) * (entries.ndim - 1 - axis_at))

    one_side = jax.random.permutation(stream_key, shards_of)[block_of(target)]
    second = (block_of(target) + shards_of // 2) % shards_of
    return jnp.where((block_of(source) == one_side) | (block_of(source) == second), factor * entries, entries)


def block_scale(stream_key, extent, cuts, smallest, largest):
    def one(dim, parts):
        steps = jax.random.uniform(jax.random.fold_in(jax.random.fold_in(stream_key, 6), dim), (parts,), jnp.float32, smallest / len(cuts), largest / len(cuts))
        return jnp.repeat(jnp.exp(steps), extent[dim] // parts).reshape((-1,) + (1,) * (len(extent) - dim - 1))

    level = one(*cuts[0])
    for cut in cuts[1:]:
        level = level * one(*cut)
    return level


def noise(own_key, extent, scale, bound, pieces=(), held_as=jnp.bfloat16):
    entries = jax.random.normal(own_key, extent, jnp.float32) * scale
    if len(pieces) > 0:
        entries = block_scale(own_key, extent, pieces, -0.22, 0.18) * entries
    return jnp.clip(entries, min=-bound, max=bound).astype(held_as)


def noise_with(stream_key, shape, width, limit, shards, heavy, kind=jnp.bfloat16):
    values = width * jax.random.normal(stream_key, shape, jnp.float32)
    if shards:
        values = values * block_scale(stream_key, shape, shards, -0.22, 0.18)
    return jnp.clip(raised(values, jax.random.fold_in(stream_key, 3), *heavy), -limit, limit).astype(kind)


def setup_inputs(seed: int = 0) -> dict:
    key_of = jax.random.split(jax.random.key(seed), 8)
    return {
        "density": jnp.clip(jnp.exp(math.log(2.0) - 1.3862944 * jax.random.uniform(key_of[0], (NX, NY, NZ), jnp.float32) ** block_scale(key_of[0], (NX, NY, NZ), ((0, 8), (1, 4), (2, 8)), -0.2, 0.2)), 0.5, 2.0),
        "velocity": noise(key_of[1], (3, NX, NY, NZ), 0.8, 3.2, ((1, 8), (2, 4), (3, 8)), jnp.float32),
        "pressure": jnp.clip(jnp.exp(math.log(2.0) - 1.3862944 * jax.random.uniform(key_of[2], (NX, NY, NZ), jnp.float32) ** block_scale(key_of[2], (NX, NY, NZ), ((0, 8), (1, 4), (2, 8)), -0.2, 0.2)), 0.5, 2.0),
        "blending": jnp.clip(0.6 * jax.random.uniform(key_of[3], (ELEMENTS_FIRST, ELEMENTS_SECOND, ELEMENTS_THIRD), jnp.float32) ** block_scale(key_of[3], (ELEMENTS_FIRST, ELEMENTS_SECOND, ELEMENTS_THIRD), ((0, 8), (1, 4), (2, 8)), -0.2, 0.2), 0.0, 0.6),
        "face_signal_weights": noise_with(key_of[4], (QN, FACES, SIG), (16 * QN * FACES) ** -0.5, 0.013671875, ((1, 32), (2, 8)), (1, 2, 32, 2.75)),
        "surf_id": draw_surf_id(jax.random.fold_in(key_of[7], 71), 0),
        "surface_face_code": draw_surface_face_code(jax.random.fold_in(key_of[7], 71), 0),
    }


GAMMA = 1.4

def gauss_lobatto():
    inner_root = math.sqrt(3.0 / 7.0)
    points = np.array([-1.0, -inner_root, 0.0, inner_root, 1.0])
    quad_weights = np.array([0.1, 49.0 / 90.0, 32.0 / 45.0, 49.0 / 90.0, 0.1])
    barycentric = np.ones(5)
    for target in range(5):
        for source in range(5):
            if source != target:
                barycentric[target] = barycentric[target] / (points[target] - points[source])
    derivative = np.zeros((5, 5))
    for target in range(5):
        for source in range(5):
            if source != target:
                derivative[target, source] = barycentric[source] / barycentric[target] / (points[target] - points[source])
        derivative[target, target] = -np.sum(derivative[target])
    return (derivative, quad_weights)

def energy_of(prim):
    speed_square = prim[1] * prim[1] + prim[2] * prim[2] + prim[3] * prim[3]
    return prim[4] / (GAMMA - 1.0) + 0.5 * prim[0] * speed_square

def conserved(prim):
    return jnp.stack([prim[0], prim[0] * prim[1], prim[0] * prim[2], prim[0] * prim[3], energy_of(prim)])

def physical_flux(prim, normal):
    mass_flux = prim[0] * prim[normal]
    flux_parts = [mass_flux]
    for field_component in (1, 2, 3):
        momentum = mass_flux * prim[field_component]
        if field_component == normal:
            momentum = momentum + prim[4]
        flux_parts.append(momentum)
    flux_parts.append((energy_of(prim) + prim[4]) * prim[normal])
    return jnp.stack(flux_parts)

def wave_speed(prim, normal):
    return jnp.abs(prim[normal]) + jnp.sqrt(GAMMA * prim[4] / prim[0])

def rusanov(left, right, normal):
    fastest = jnp.maximum(wave_speed(left, normal), wave_speed(right, normal))
    return 0.5 * (physical_flux(left, normal) + physical_flux(right, normal)) - 0.5 * fastest * (conserved(right) - conserved(left))

def split_flux(left, right, normal):
    density = 0.5 * (left[0] + right[0])
    pressure = 0.5 * (left[4] + right[4])
    mean_normal = 0.5 * (left[normal] + right[normal])
    specific = 0.5 * (energy_of(left) / left[0] + energy_of(right) / right[0])
    mass_flux = density * mean_normal
    flux_parts = [mass_flux]
    for field_component in (1, 2, 3):
        momentum = mass_flux * (0.5 * (left[field_component] + right[field_component]))
        if field_component == normal:
            momentum = momentum + pressure
        flux_parts.append(momentum)
    flux_parts.append(mass_flux * specific + pressure * mean_normal)
    return jnp.stack(flux_parts)

def direction_terms(core, lower, upper, node_factors, axis_dim):
    derivative, quad_weights = gauss_lobatto()
    node_count = derivative.shape[0]
    full_shape = core.shape
    elem_count = full_shape[axis_dim] // node_count
    split_shape = full_shape[:axis_dim] + (elem_count, node_count) + full_shape[axis_dim + 1:]
    ghost_shape = full_shape[:axis_dim] + (1, 1) + full_shape[axis_dim + 1:]
    node_axis = axis_dim + 1
    node_shape = [1] * len(split_shape)
    node_shape[node_axis] = node_count
    node_shape = tuple(node_shape)
    by_element = core.reshape(split_shape)
    blend_split = node_factors.reshape(split_shape[1:])[None]
    high_order = jnp.zeros(split_shape, jnp.float32)
    for column in range(node_count):
        partner = lax.slice_in_dim(by_element, column, column + 1, axis=node_axis)
        factor = jnp.asarray(2.0 * derivative[:, column], jnp.float32).reshape(node_shape)
        high_order = high_order + factor * split_flux(by_element, partner, axis_dim)
    node_flux = physical_flux(by_element, axis_dim)
    inner_flux = rusanov(lax.slice_in_dim(by_element, 0, node_count - 1, axis=node_axis), lax.slice_in_dim(by_element, 1, node_count, axis=node_axis), axis_dim)
    edge_flux = jnp.concatenate([lax.slice_in_dim(node_flux, 0, 1, axis=node_axis), inner_flux, lax.slice_in_dim(node_flux, node_count - 1, node_count, axis=node_axis)], axis=node_axis)
    weight_row = jnp.asarray(quad_weights, jnp.float32).reshape(node_shape)
    low_order = (lax.slice_in_dim(edge_flux, 1, node_count + 1, axis=node_axis) - lax.slice_in_dim(edge_flux, 0, node_count, axis=node_axis)) / weight_row
    volume = high_order + blend_split * (low_order - high_order)
    first_nodes = lax.slice_in_dim(by_element, 0, 1, axis=node_axis)
    last_nodes = lax.slice_in_dim(by_element, node_count - 1, node_count, axis=node_axis)
    left_states = jnp.concatenate([lower.reshape(ghost_shape), last_nodes], axis=axis_dim)
    right_states = jnp.concatenate([first_nodes, upper.reshape(ghost_shape)], axis=axis_dim)
    face_flux = rusanov(left_states, right_states, axis_dim)
    lower_term = -(lax.slice_in_dim(face_flux, 0, elem_count, axis=axis_dim) - lax.slice_in_dim(node_flux, 0, 1, axis=node_axis)) / float(quad_weights[0])
    upper_term = (lax.slice_in_dim(face_flux, 1, elem_count + 1, axis=axis_dim) - lax.slice_in_dim(node_flux, node_count - 1, node_count, axis=node_axis)) / float(quad_weights[-1])
    middle_shape = list(split_shape)
    middle_shape[node_axis] = node_count - 2
    surface = jnp.concatenate([lower_term, jnp.zeros(tuple(middle_shape), jnp.float32), upper_term], axis=node_axis)
    return (volume + surface).reshape(full_shape)

def tendency_of(core, ghosts, node_factors):
    running = jnp.zeros(core.shape, jnp.float32)
    for axis_dim in (1, 2, 3):
        running = running - direction_terms(core, ghosts[axis_dim - 1][0], ghosts[axis_dim - 1][1], node_factors, axis_dim)
    return running

def node_blend(blend_factors, node_count):
    first_count, second_count, third_count = blend_factors.shape
    widened = jnp.broadcast_to(blend_factors[:, None, :, None, :, None], (first_count, node_count, second_count, node_count, third_count, node_count))
    return widened.reshape(first_count * node_count, second_count * node_count, third_count * node_count)

def face_sources(values, face_code, elem_total):
    face_index = face_code // elem_total
    normal_dim = face_index // 2
    sign = (2 * (face_index % 2) - 1).astype(jnp.float32)
    picks = (normal_dim[:, None] == jnp.arange(3, dtype=jnp.int32)[None, :]).astype(jnp.float32)
    normal_speed = sign[:, None] * (picks[:, 0:1] * values[1] + picks[:, 1:2] * values[2] + picks[:, 2:3] * values[3])
    quad_weights = gauss_lobatto()[1]
    surface_weights = jnp.asarray(np.outer(quad_weights, quad_weights).reshape(-1), jnp.float32)
    mass_flux = values[0] * normal_speed
    quantities = [mass_flux]
    for field_component in (1, 2, 3):
        quantities.append(values[4] * (sign[:, None] * picks[:, field_component - 1:field_component]) + mass_flux * values[field_component])
    return jnp.stack([lax.optimization_barrier(jnp.sum(surface_weights * amount, axis=1)) for amount in quantities])

def reference(density, velocity, pressure, blending, face_signal_weights, surf_id, surface_face_code):
    primitive = jnp.concatenate([density[None], velocity, pressure[None]], axis=0)
    node_count = 5
    wrapped_around = jnp.concatenate([primitive[:, -1:], primitive, primitive[:, :1]], axis=1)

    def slab_terms(slab_index):
        window = lax.dynamic_slice_in_dim(wrapped_around, slab_index * node_count, node_count + 2, 1)
        slab_core = window[:, 1:-1]
        ghosts = ((window[:, 0:1], window[:, -1:]), (slab_core[:, :, -1:], slab_core[:, :, :1]), (slab_core[:, :, :, -1:], slab_core[:, :, :, :1]))
        node_factors = node_blend(lax.dynamic_slice_in_dim(blending, slab_index, 1, 0), node_count)
        return tendency_of(slab_core, ghosts, node_factors)
    slab_all = lax.map(slab_terms, jnp.arange(ELEMENTS_FIRST, dtype=jnp.int32))
    tendency = jnp.transpose(slab_all, (1, 0, 2, 3, 4)).reshape(primitive.shape)
    slot_total = surface_face_code.shape[0]
    slot_index = jnp.arange(slot_total, dtype=jnp.int32)
    device = slot_index // SLOTS
    owner_x = device // (N_GY * N_GZ)
    owner_y = device // N_GZ % N_GY
    owner_z = device % N_GZ
    elem_total = EX * EY * EZ
    face_index = surface_face_code // elem_total
    mesh_element = surface_face_code % elem_total
    elem_x = owner_x * EX + mesh_element // (EY * EZ)
    elem_y = owner_y * EY + mesh_element // EZ % EY
    elem_z = owner_z * EZ + mesh_element % EZ
    normal_dim = (face_index // 2)[:, None, None]
    fixed_node = (face_index % 2 * (node_count - 1))[:, None, None]
    across_first = jnp.arange(node_count, dtype=jnp.int32)[None, :, None]
    across_second = jnp.arange(node_count, dtype=jnp.int32)[None, None, :]
    base_x = (elem_x * node_count)[:, None, None]
    base_y = (elem_y * node_count)[:, None, None]
    base_z = (elem_z * node_count)[:, None, None]
    index_x = jnp.where(normal_dim == 0, base_x + fixed_node, base_x + across_first)
    index_y = jnp.where(normal_dim == 0, base_y + across_first, jnp.where(normal_dim == 1, base_y + fixed_node, base_y + across_second))
    index_z = jnp.where(normal_dim == 2, base_z + fixed_node, base_z + across_second)
    values = primitive[:, index_x, index_y, index_z].reshape(5, slot_total, node_count * node_count)
    face_data = face_sources(values, surface_face_code, elem_total).astype(jnp.bfloat16)
    placed = jnp.where(surf_id >= 0, surf_id, FACES).astype(jnp.int32)
    surface_data = jnp.zeros((QN, FACES), jnp.bfloat16).at[:, placed].set(face_data, mode='drop')
    group_faces = FACES // (N_GX * N_GY)

    def add_group(group_index, running):
        first_face = (group_index * group_faces).astype(jnp.int32)
        data_block = lax.dynamic_slice_in_dim(surface_data, first_face, group_faces, 1).reshape(-1)
        weight_block = lax.dynamic_slice_in_dim(face_signal_weights, first_face, group_faces, 1).reshape(QN * group_faces, SIG)
        return running + jnp.dot(data_block, weight_block, preferred_element_type=jnp.float32)
    signals = lax.fori_loop(0, N_GX * N_GY, add_group, jnp.zeros((SIG,), jnp.float32))
    return (tendency, signals)
```

```python
import functools
import math

import jax
import jax.numpy as jnp
import numpy as np
from jax import lax
from jax.experimental import pallas as pl
from jax.experimental.pallas import tpu as pltpu
from jax.sharding import PartitionSpec as P

GAMMA = 1.4
NODES = 5
PAIR = ("gx", "gy")
LANES = 256
F32 = jnp.float32
BF16 = jnp.bfloat16


def gauss_lobatto():
    inner_root = math.sqrt(3.0 / 7.0)
    points = np.array([-1.0, -inner_root, 0.0, inner_root, 1.0])
    quad_weights = np.array([0.1, 49.0 / 90.0, 32.0 / 45.0, 49.0 / 90.0, 0.1])
    barycentric = np.ones(5)
    for target in range(5):
        for source in range(5):
            if source != target:
                barycentric[target] = barycentric[target] / (points[target] - points[source])
    derivative = np.zeros((5, 5))
    for target in range(5):
        for source in range(5):
            if source != target:
                derivative[target, source] = (
                    barycentric[source] / barycentric[target] / (points[target] - points[source])
                )
        derivative[target, target] = -np.sum(derivative[target])
    return (derivative, quad_weights)


DERIV, WEIGHTS = gauss_lobatto()


def iota(shape, dim):
    return lax.broadcasted_iota(jnp.int32, shape, dim)


def by_node(node, values):
    picked = jnp.zeros(node.shape, F32)
    for n, value in enumerate(values):
        if value != 0.0:
            picked = jnp.where(node == n, F32(value), picked)
    return picked


def flux4(rho, vel, pressure, d):
    mass = rho * vel[d]
    return [mass] + [mass * vel[m] + pressure if m == d else mass * vel[m] for m in range(3)]


def face_kernel(per_group, den, vel, pre, sid, code, blocks, x_lo, x_hi, y_lo, y_hi, z_lo, z_hi, rows):
    nx, ny, nz = den.shape
    slots = sid.shape[1]
    groups = blocks.shape[0]
    fields = lambda x: (den[x], [vel[m, x] for m in range(3)], pre[x])
    wy = by_node(iota((ny, nz), 0), WEIGHTS)

    for f in range(5):
        ref = den if f == 0 else pre if f == 4 else vel.at[f - 1]
        x_lo[f] = ref[0]
        x_hi[f] = ref[nx - 1]
        for x in range(nx):
            y_lo[f, x : x + 1] = ref[x, 0:1]
            y_hi[f, x : x + 1] = ref[x, ny - 1 : ny]

    rows[...] = jnp.zeros_like(rows)
    sum_y = [None] * 4
    sum_z = [None] * 4
    for x in range(nx):
        rho, v, p = fields(x)
        for q, value in enumerate(flux4(rho, v, p, 1)):
            term = F32(WEIGHTS[x]) * value
            sum_y[q] = term if sum_y[q] is None else sum_y[q] + term
        for q, value in enumerate(flux4(rho, v, p, 2)):
            term = F32(WEIGHTS[x]) * value
            sum_z[q] = term if sum_z[q] is None else sum_z[q] + term
        if x in (0, nx - 1):
            side, sign = (0, -1.0) if x == 0 else (1, 1.0)
            for q, value in enumerate(flux4(rho, v, p, 0)):
                rows[8 * q + side : 8 * q + side + 1, :] = F32(sign) * jnp.sum(wy * value, axis=0, keepdims=True)
    for q in range(4):
        rows[8 * q + 2 : 8 * q + 3, :] = -sum_y[q][0:1]
        rows[8 * q + 3 : 8 * q + 4, :] = sum_y[q][ny - 1 : ny]
        over_z = jnp.sum(wy * sum_z[q], axis=0, keepdims=True)
        rows[8 * q + 4 : 8 * q + 5, :] = -over_z
        rows[8 * q + 5 : 8 * q + 6, :] = over_z

    face = lax.shift_right_logical(code[...], 5)
    elem = code[...] & 31
    z = iota((nz, slots), 0)
    z_elem = lax.shift_right_logical(z * 52429, 18)
    z_node = z - 5 * z_elem
    plane = jnp.where(z_node == 4 * (face - 4), F32(1), F32(0))
    pick = jnp.where(z_elem == elem, jnp.where(face < 4, by_node(z_node, WEIGHTS), plane), F32(0))
    by_face = jnp.dot(rows[...], pick, precision=lax.Precision.HIGHEST, preferred_element_type=F32)
    face_hot = iota((8, slots), 0) == face
    data = [
        jnp.sum(jnp.where(face_hot, by_face[8 * q : 8 * q + 8], F32(0)), axis=0, keepdims=True)
        for q in range(4)
    ]

    ids = sid[...]
    group = lax.shift_right_logical(jnp.maximum(ids, 0) * 6554, 21)
    offset = ids - per_group * group
    chunk = lax.shift_right_logical(jnp.maximum(offset, 0), 7)
    group = jnp.where(ids >= 0, group, -1)
    row = iota((16, slots), 0)
    row_q = lax.shift_right_logical(row * 21846, 16)
    spread = jnp.zeros((16, slots), F32)
    for q in range(4):
        spread = jnp.where(row_q == q, data[q], spread)
    spread = jnp.where(row - 3 * row_q == chunk, spread, F32(0)).astype(BF16).astype(F32)
    group_of = iota((groups, 16, slots), 0)
    spread = jnp.where(group_of == group[None], spread[None], F32(0))
    spread = spread.reshape(groups * 16, slots).astype(BF16)
    lane_hot = (iota((128, slots), 0) == (offset & 127)).astype(F32).astype(BF16)
    placed = lax.dot_general(spread, lane_hot, (((1,), (1,)), ((), ())), preferred_element_type=F32)
    blocks[...] = placed.astype(BF16).reshape(groups, 16, 128)

    lane = iota((8, 128), 1)
    low = jnp.zeros((8, 128), F32)
    high = jnp.zeros((8, 128), F32)
    z_lo[...] = low
    z_hi[...] = high
    low = jnp.zeros((ny, 128), F32)
    high = jnp.zeros((ny, 128), F32)
    lane = iota((ny, 128), 1)
    for f in range(5):
        ref = den if f == 0 else pre if f == 4 else vel.at[f - 1]
        for x in range(nx):
            at = 5 * f + x
            low = jnp.where(lane == at, ref[x, :, 0:1], low)
            high = jnp.where(lane == at, ref[x, :, nz - 1 : nz], high)
    z_lo[0:ny] = low
    z_hi[0:ny] = high


def split_flux(a, b, d):
    half = [F32(0.5) * (x + y) for x, y in zip(a, b)]
    rho, vel, pressure, specific = half[0], half[1:4], half[4], half[5]
    mass = rho * vel[d]
    out = [mass]
    for m in range(3):
        value = mass * vel[m]
        out.append(value + pressure if m == d else value)
    out.append(mass * specific + pressure * vel[d])
    return out


def node_parts(a, d):
    rho, vel, pressure, specific, sound = a[0], a[1:4], a[4], a[5], a[6]
    cons = [rho] + [rho * v for v in vel] + [rho * specific]
    mass = cons[1 + d]
    flux = [mass] + [mass * vel[m] + pressure if m == d else mass * vel[m] for m in range(3)]
    flux.append((cons[4] + pressure) * vel[d])
    return flux, cons, jnp.abs(vel[d]) + sound


def rusanov(left, right):
    speed = F32(0.5) * jnp.maximum(left[2], right[2])
    return [
        F32(0.5) * (fl + fr) - speed * (ur - ul)
        for fl, fr, ul, ur in zip(left[0], right[0], left[1], right[1])
    ]


def derived(rho, v1, v2, v3, pressure):
    inverse = F32(1) / rho
    ratio = pressure * inverse
    specific = ratio * F32(1.0 / (GAMMA - 1.0)) + F32(0.5) * (v1 * v1 + v2 * v2 + v3 * v3)
    return [rho, v1, v2, v3, pressure, specific, jnp.sqrt(F32(GAMMA) * ratio)]


def tendency_kernel(
    den, vel, pre, blend, x_low, x_up, y_low, y_up, z_low, z_up, out, grid
):
    nx, ny, nz = den.shape
    shape = (8, LANES)
    grid[...] = jnp.ones_like(grid)
    half_lane = iota((8, 128), 1)
    for f in range(5):
        ref = den if f == 0 else pre if f == 4 else vel.at[f - 1]
        grid[f, 0, 0:ny, 0:nz] = x_low[f]
        grid[f, 1 + nx, 0:ny, 0:nz] = x_up[f]
        for x in range(nx):
            grid[f, 1 + x, 0:ny, 0:nz] = ref[x]
            grid[f, 1 + x, ny : ny + 1, 0:nz] = y_up[f, x : x + 1]
            grid[f, 1 + x, 7:8, 0:nz] = y_low[f, x : x + 1]
            at = 5 * f + x
            upper = grid[f, 1 + x, :, 128:256]
            upper = jnp.where(half_lane == nz - 128, pltpu.roll(z_up[...], (nz - 128 - at) % 128, 1), upper)
            upper = jnp.where(half_lane == 127, pltpu.roll(z_low[...], (127 - at) % 128, 1), upper)
            upper = jnp.where((iota((8, 128), 0) >= ny) & (half_lane >= nz - 128), F32(1), upper)
            grid[f, 1 + x, :, 128:256] = upper

    def state(x):
        return derived(*[grid[f, 1 + x] for f in range(5)])

    row = iota(shape, 0)
    lane = iota(shape, 1)
    lane_elem = lax.shift_right_logical(lane * 52429, 18)
    node = lane - 5 * lane_elem
    elems = blend.shape[1]
    spread = (iota((elems, LANES), 0) == lax.shift_right_logical(iota((elems, LANES), 1) * 52429, 18)).astype(F32)
    alpha = jnp.dot(
        jnp.broadcast_to(blend[...], (8, elems)), spread, precision=lax.Precision.HIGHEST, preferred_element_type=F32
    )
    keep = F32(1) - alpha
    inv = 1.0 / WEIGHTS

    def sides(index):
        inverse = by_node(index, inv)
        up = inverse * jnp.where(index == NODES - 1, F32(1), alpha)
        low = inverse * jnp.where(index == 0, F32(1), alpha)
        return up, low

    def pair_factors(index):
        ups = [by_node(index, [2.0 * DERIV[i, i + k] if i + k < NODES else 0.0 for i in range(NODES)]) for k in range(1, NODES)]
        downs = [by_node(index, [2.0 * DERIV[i, i - k] if i >= k else 0.0 for i in range(NODES)]) for k in range(1, NODES)]
        return ups, downs

    states = [state(x) for x in range(-1, nx + 1)]
    parts = [node_parts(s, 0) for s in states]
    faces = [rusanov(parts[i], parts[i + 1]) for i in range(nx + 1)]
    high = [[None] * 5 for _ in range(nx)]
    for i in range(nx):
        for j in range(i + 1, nx):
            pair = split_flux(states[1 + i], states[1 + j], 0)
            for c in range(5):
                for target, source in ((i, j), (j, i)):
                    term = F32(2.0 * DERIV[target, source]) * pair[c]
                    high[target][c] = term if high[target][c] is None else high[target][c] + term
    total = [[None] * 5 for _ in range(nx)]
    for x in range(nx):
        up = F32(inv[x]) if x == nx - 1 else F32(inv[x]) * alpha
        low = F32(inv[x]) if x == 0 else F32(inv[x]) * alpha
        for c in range(5):
            total[x][c] = keep * high[x][c] + (up * faces[x + 1][c] - low * faces[x][c])

    for d, axis, size, index in ((1, 0, 8, row), (2, 1, LANES, node)):
        ups, downs = pair_factors(index)
        up, low = sides(index)
        for x in range(nx):
            here = states[1 + x]
            high_x = [None] * 5
            for k in range(1, NODES):
                there = [pltpu.roll(s, size - k, axis) for s in (here if k == 1 else here[:6])]
                pair = split_flux(here[:6], there[:6], d)
                for c in range(5):
                    term = ups[k - 1] * pair[c] + downs[k - 1] * pltpu.roll(pair[c], k, axis)
                    high_x[c] = term if high_x[c] is None else high_x[c] + term
                if k == 1:
                    face = rusanov(node_parts(here, d), node_parts(there, d))
                    edge = [up * f - low * pltpu.roll(f, 1, axis) for f in face]
            for c in range(5):
                total[x][c] = total[x][c] + (keep * high_x[c] + edge[c])
    for x in range(nx):
        for c in range(5):
            out[c, x] = (-total[x][c])[0:ny, 0:nz]


def gather_kernel(got, copies):
    total = got[0].astype(F32)
    for i in range(1, got.shape[0]):
        total = total + got[i].astype(F32)
    total = total.astype(BF16)
    for i in range(copies.shape[0]):
        copies[i] = total


def signal_kernel(got, weights, out):
    blocks = jnp.zeros((got.shape[0], weights.shape[2]), F32)
    faces = weights.shape[1]
    for q in range(weights.shape[0]):
        for c in range(3):
            width = min(128, faces - 128 * c)
            data = got[:, 3 * q + c, 0:width]
            blocks = blocks + jnp.dot(data, weights[q, 128 * c : 128 * c + width, :], preferred_element_type=F32)
    out[...] = jnp.sum(blocks, axis=0, keepdims=True)


def vmem(n):
    return [pl.BlockSpec(memory_space=pltpu.VMEM)] * n


def call(kernel, outs, args, scratch=(), flops=1_000_000):
    single = not isinstance(outs, (list, tuple))
    return pl.pallas_call(
        kernel,
        out_shape=outs,
        in_specs=vmem(len(args)),
        out_specs=vmem(1)[0] if single else vmem(len(outs)),
        scratch_shapes=scratch,
        compiler_params=pltpu.CompilerParams(vmem_limit_bytes=16 * 1024 * 1024),
        cost_estimate=pl.CostEstimate(flops=flops, bytes_accessed=200_000, transcendentals=0),
    )(*args)


def shards(density, velocity, pressure, blending, face_signal_weights, surf_id, surface_face_code):
    nx, ny, nz = density.shape
    sds = jax.ShapeDtypeStruct
    groups = lax.axis_size("gx") * lax.axis_size("gy")
    layers = lax.axis_size("gz")
    quantities, faces, local = face_signal_weights.shape
    ids = surf_id.reshape(1, -1)
    codes = surface_face_code.reshape(1, -1)
    blocks, x_lo, x_hi, y_lo, y_hi, z_lo, z_hi = call(
        functools.partial(face_kernel, faces),
        [sds((groups, 16, 128), BF16)]
        + [sds((5, ny, nz), F32)] * 2
        + [sds((5, nx, nz), F32)] * 2
        + [sds((8, 128), F32)] * 2,
        [density, velocity, pressure, ids, codes],
        [pltpu.VMEM((32, nz), F32)],
    )
    arrived = lax.all_to_all(blocks, PAIR, 0, 0, tiled=True)

    def shift(array, axis, step):
        peers = lax.axis_size(axis)
        return lax.ppermute(array, axis, [(i, (i + step) % peers) for i in range(peers)])

    x_low, x_up = shift(x_hi, "gx", 1), shift(x_lo, "gx", -1)
    y_low, y_up = shift(y_hi, "gy", 1), shift(y_lo, "gy", -1)
    z_low, z_up = shift(z_hi, "gz", 1), shift(z_lo, "gz", -1)

    copies = call(gather_kernel, sds((layers, 16, 128), BF16), [arrived])
    everywhere = lax.all_to_all(copies, "gz", 0, 0, tiled=True)
    partial = call(signal_kernel, sds((1, local), F32), [everywhere, face_signal_weights])
    tiles = lax.all_to_all(partial.reshape(groups, local // groups), PAIR, 0, 0, tiled=True)
    signals = jnp.sum(tiles, axis=0)

    tendency = call(
        tendency_kernel,
        sds((5, nx, ny, nz), F32),
        [density, velocity, pressure, blending.reshape(1, -1), x_low, x_up, y_low, y_up, z_low, z_up],
        [pltpu.VMEM((5, nx + 2, 8, LANES), F32)],
        flops=20_000_000,
    )
    return (tendency, signals)


def solution(mesh):
    placed = (
        P("gx", "gy", "gz"),
        P(None, "gx", "gy", "gz"),
        P("gx", "gy", "gz"),
        P("gx", "gy", "gz"),
        P(None, ("gx", "gy"), "gz"),
        P(("gx", "gy", "gz")),
        P(("gx", "gy", "gz")),
    )
    return jax.shard_map(
        shards,
        mesh=mesh,
        in_specs=placed,
        out_specs=(P(None, "gx", "gy", "gz"), P(("gz", "gx", "gy"))),
        check_vma=False,
    )
```

```python
import functools
import math

import jax
import jax.numpy as jnp
import numpy as np
from jax import lax
from jax.experimental import pallas as pl
from jax.experimental.pallas import tpu as pltpu
from jax.sharding import PartitionSpec as P


GAMMA = 1.4
NODES = 5
PAIR = ("gx", "gy")
LANES = 256
F32 = jnp.float32
BF16 = jnp.bfloat16


def gauss_lobatto():
    inner_root = math.sqrt(3.0 / 7.0)
    points = np.array([-1.0, -inner_root, 0.0, inner_root, 1.0])
    quad_weights = np.array([0.1, 49.0 / 90.0, 32.0 / 45.0, 49.0 / 90.0, 0.1])
    barycentric = np.ones(5)
    for target in range(5):
        for source in range(5):
            if source != target:
                barycentric[target] = barycentric[target] / (points[target] - points[source])
    derivative = np.zeros((5, 5))
    for target in range(5):
        for source in range(5):
            if source != target:
                derivative[target, source] = (
                    barycentric[source] / barycentric[target] / (points[target] - points[source])
                )
        derivative[target, target] = -np.sum(derivative[target])
    return (derivative, quad_weights)


DERIV, WEIGHTS = gauss_lobatto()


def iota(shape, dim):
    return lax.broadcasted_iota(jnp.int32, shape, dim)


def by_node(node, values):
    picked = jnp.zeros(node.shape, F32)
    for n, value in enumerate(values):
        if value != 0.0:
            picked = jnp.where(node == n, F32(value), picked)
    return picked


def flux4(rho, vel, pressure, d):
    mass = rho * vel[d]
    return [mass] + [mass * vel[m] + pressure if m == d else mass * vel[m] for m in range(3)]


def lay_out(den, vel, pre, grid):
    nx, ny, nz = den.shape
    for x in range(nx):
        grid[0, x, 0:ny, 0:nz] = den[x]
        grid[4, x, 0:ny, 0:nz] = pre[x]
        for y in range(ny):
            for m in range(3):
                grid[1 + m, x, y : y + 1, 0:nz] = vel[x, y, m : m + 1, :]


def face_kernel(per_group, den, vel, pre, sid, code, blocks, x_lo, x_hi, y_lo, y_hi, z_both, grid, rows, den_v, vel_v, pre_v, sid_v, code_v, sems):
    pairs = ((den, den_v), (vel, vel_v), (pre, pre_v), (sid, sid_v), (code, code_v))
    loads = [pltpu.make_async_copy(src, dst, sems.at[i]) for i, (src, dst) in enumerate(pairs)]
    for load in loads:
        load.start()
    nx, ny, nz = den.shape
    slots = sid.shape[1]
    groups = blocks.shape[0]
    rows[...] = jnp.zeros_like(rows)
    for load in loads:
        load.wait()

    lay_out(den_v, vel_v, pre_v, grid)

    def field(f, x):
        return grid[f, x, 0:ny, 0:nz]

    wy = by_node(iota((ny, nz), 0), WEIGHTS)

    sum_y = [None] * 4
    sum_z = [None] * 4
    for x in range(nx):
        rho, v, p = field(0, x), [field(1 + m, x) for m in range(3)], field(4, x)
        for q, value in enumerate(flux4(rho, v, p, 1)):
            term = F32(WEIGHTS[x]) * value
            sum_y[q] = term if sum_y[q] is None else sum_y[q] + term
        for q, value in enumerate(flux4(rho, v, p, 2)):
            term = F32(WEIGHTS[x]) * value
            sum_z[q] = term if sum_z[q] is None else sum_z[q] + term
        if x in (0, nx - 1):
            side, sign = (0, -1.0) if x == 0 else (1, 1.0)
            for q, value in enumerate(flux4(rho, v, p, 0)):
                rows[8 * q + side : 8 * q + side + 1, :] = F32(sign) * jnp.sum(wy * value, axis=0, keepdims=True)
    for q in range(4):
        rows[8 * q + 2 : 8 * q + 3, :] = -sum_y[q][0:1]
        rows[8 * q + 3 : 8 * q + 4, :] = sum_y[q][ny - 1 : ny]
        over_z = jnp.sum(wy * sum_z[q], axis=0, keepdims=True)
        rows[8 * q + 4 : 8 * q + 5, :] = -over_z
        rows[8 * q + 5 : 8 * q + 6, :] = over_z

    face = lax.shift_right_logical(code_v[...], 5)
    elem = code_v[...] & 31
    z = iota((nz, slots), 0)
    z_elem = lax.shift_right_logical(z * 52429, 18)
    z_node = z - 5 * z_elem
    plane = jnp.where(z_node == 4 * (face - 4), F32(1), F32(0))
    pick = jnp.where(z_elem == elem, jnp.where(face < 4, by_node(z_node, WEIGHTS), plane), F32(0))
    by_face = jnp.dot(rows[...], pick, precision=lax.Precision.HIGHEST, preferred_element_type=F32)
    face_hot = iota((8, slots), 0) == face
    data = [
        jnp.sum(jnp.where(face_hot, by_face[8 * q : 8 * q + 8], F32(0)), axis=0, keepdims=True)
        for q in range(4)
    ]

    ids = sid_v[...]
    group = lax.shift_right_logical(jnp.maximum(ids, 0) * 6554, 21)
    offset = ids - per_group * group
    chunk = lax.shift_right_logical(jnp.maximum(offset, 0), 7)
    group = jnp.where(ids >= 0, group, -1)
    row = iota((16, slots), 0)
    row_q = lax.shift_right_logical(row * 21846, 16)
    spread = jnp.zeros((16, slots), F32)
    for q in range(4):
        spread = jnp.where(row_q == q, data[q], spread)
    spread = jnp.where(row - 3 * row_q == chunk, spread, F32(0)).astype(BF16).astype(F32)
    group_of = iota((groups, 16, slots), 0)
    spread = jnp.where(group_of == group[None], spread[None], F32(0))
    spread = spread.reshape(groups * 16, slots).astype(BF16)
    lane_hot = (iota((128, slots), 0) == (offset & 127)).astype(F32).astype(BF16)
    placed = lax.dot_general(spread, lane_hot, (((1,), (1,)), ((), ())), preferred_element_type=F32)
    blocks[...] = placed.astype(BF16).reshape(groups, 16, 128)

    for f in range(5):
        x_lo[f] = grid[f, 0, 0:ny, 0:nz]
        x_hi[f] = grid[f, nx - 1, 0:ny, 0:nz]
        for x in range(nx):
            y_lo[f, x : x + 1] = grid[f, x, 0:1, 0:nz]
            y_hi[f, x : x + 1] = grid[f, x, ny - 1 : ny, 0:nz]

    z_both[...] = jnp.zeros_like(z_both)
    packed = jnp.zeros((ny, 128), F32)
    lane = iota((ny, 128), 1)
    for f in range(5):
        for x in range(nx):
            at = 5 * f + x
            packed = jnp.where(lane == at, grid[f, x, 0:ny, 0:1], packed)
            packed = jnp.where(lane == 64 + at, grid[f, x, 0:ny, nz - 1 : nz], packed)
    z_both[0:ny] = packed


def split_flux(a, b, d):
    half = [F32(0.5) * (x + y) for x, y in zip(a, b)]
    rho, vel, pressure, specific = half[0], half[1:4], half[4], half[5]
    mass = rho * vel[d]
    out = [mass]
    for m in range(3):
        value = mass * vel[m]
        out.append(value + pressure if m == d else value)
    out.append(mass * specific + pressure * vel[d])
    return out


def node_parts(a, d):
    rho, vel, pressure, specific, sound = a[0], a[1:4], a[4], a[5], a[6]
    cons = [rho] + [rho * v for v in vel] + [rho * specific]
    mass = cons[1 + d]
    flux = [mass] + [mass * vel[m] + pressure if m == d else mass * vel[m] for m in range(3)]
    flux.append((cons[4] + pressure) * vel[d])
    return flux, cons, jnp.abs(vel[d]) + sound


def rusanov(left, right):
    speed = F32(0.5) * jnp.maximum(left[2], right[2])
    return [
        F32(0.5) * (fl + fr) - speed * (ur - ul)
        for fl, fr, ul, ur in zip(left[0], right[0], left[1], right[1])
    ]


def derived(rho, v1, v2, v3, pressure):
    inverse = F32(1) / rho
    ratio = pressure * inverse
    specific = ratio * F32(1.0 / (GAMMA - 1.0)) + F32(0.5) * (v1 * v1 + v2 * v2 + v3 * v3)
    return [rho, v1, v2, v3, pressure, specific, jnp.sqrt(F32(GAMMA) * ratio)]


def tendency_kernel(start, blend, x_low, x_up, y_low, y_up, z_all, out, grid):
    _, nx, ny, nz = out.shape
    shape = (8, LANES)
    grid[...] = jnp.ones_like(grid)
    layers = z_all.shape[0]
    here = lax.axis_index("gz")
    z_low = z_all[lax.rem(here + layers - 1, layers), 16:24]
    z_up = z_all[lax.rem(here + 1, layers), 16:24]
    half_lane = iota((8, 128), 1)
    outside = (iota((8, 128), 0) >= ny) & (half_lane >= nz - 128)
    for f in range(5):
        grid[f, 0, 0:ny, 0:nz] = x_low[f]
        grid[f, 1 + nx, 0:ny, 0:nz] = x_up[f]
        for x in range(nx):
            grid[f, 1 + x, 0:ny, 0:nz] = start[f, x, 0:ny, 0:nz]
            grid[f, 1 + x, ny : ny + 1, 0:nz] = y_up[f, x : x + 1]
            grid[f, 1 + x, 7:8, 0:nz] = y_low[f, x : x + 1]
            at = 5 * f + x
            upper = grid[f, 1 + x, :, 128:256]
            upper = jnp.where(half_lane == nz - 128, pltpu.roll(z_up, (nz - 128 - at) % 128, 1), upper)
            upper = jnp.where(half_lane == 127, pltpu.roll(z_low, (127 - 64 - at) % 128, 1), upper)
            upper = jnp.where(outside, F32(1), upper)
            grid[f, 1 + x, :, 128:256] = upper

    def state(x):
        return derived(*[grid[f, 1 + x] for f in range(5)])

    row = iota(shape, 0)
    lane = iota(shape, 1)
    lane_elem = lax.shift_right_logical(lane * 52429, 18)
    node = lane - 5 * lane_elem
    elems = blend.shape[1]
    spread = (iota((elems, LANES), 0) == lax.shift_right_logical(iota((elems, LANES), 1) * 52429, 18)).astype(F32)
    alpha = jnp.dot(
        jnp.broadcast_to(blend[...], (8, elems)), spread, precision=lax.Precision.HIGHEST, preferred_element_type=F32
    )
    keep = F32(1) - alpha
    inv = 1.0 / WEIGHTS

    def sides(index):
        inverse = by_node(index, inv)
        up = inverse * jnp.where(index == NODES - 1, F32(1), alpha)
        low = inverse * jnp.where(index == 0, F32(1), alpha)
        return up, low

    def pair_factors(index):
        ups = [by_node(index, [2.0 * DERIV[i, i + k] if i + k < NODES else 0.0 for i in range(NODES)]) for k in range(1, NODES)]
        downs = [by_node(index, [2.0 * DERIV[i, i - k] if i >= k else 0.0 for i in range(NODES)]) for k in range(1, NODES)]
        return ups, downs

    states = [state(x) for x in range(-1, nx + 1)]
    parts = [node_parts(s, 0) for s in states]
    faces = [rusanov(parts[i], parts[i + 1]) for i in range(nx + 1)]
    high = [[None] * 5 for _ in range(nx)]
    for i in range(nx):
        for j in range(i + 1, nx):
            pair = split_flux(states[1 + i], states[1 + j], 0)
            for c in range(5):
                for target, source in ((i, j), (j, i)):
                    term = F32(2.0 * DERIV[target, source]) * pair[c]
                    high[target][c] = term if high[target][c] is None else high[target][c] + term
    total = [[None] * 5 for _ in range(nx)]
    for x in range(nx):
        up = F32(inv[x]) if x == nx - 1 else F32(inv[x]) * alpha
        low = F32(inv[x]) if x == 0 else F32(inv[x]) * alpha
        for c in range(5):
            total[x][c] = keep * high[x][c] + (up * faces[x + 1][c] - low * faces[x][c])

    for d, axis, size, index in ((1, 0, 8, row), (2, 1, LANES, node)):
        ups, downs = pair_factors(index)
        up, low = sides(index)
        for x in range(nx):
            node_here = states[1 + x]
            high_x = [None] * 5
            for k in range(1, NODES):
                there = [pltpu.roll(s, size - k, axis) for s in (node_here if k == 1 else node_here[:6])]
                pair = split_flux(node_here[:6], there[:6], d)
                for c in range(5):
                    term = ups[k - 1] * pair[c] + downs[k - 1] * pltpu.roll(pair[c], k, axis)
                    high_x[c] = term if high_x[c] is None else high_x[c] + term
                if k == 1:
                    face = rusanov(node_parts(node_here, d), node_parts(there, d))
                    edge = [up * f - low * pltpu.roll(f, 1, axis) for f in face]
            for c in range(5):
                total[x][c] = total[x][c] + (keep * high_x[c] + edge[c])
    for x in range(nx):
        for c in range(5):
            out[c, x] = (-total[x][c])[0:ny, 0:nz]


def gather_kernel(got, z_both, copies):
    total = got[0].astype(F32)
    for i in range(1, got.shape[0]):
        total = total + got[i].astype(F32)
    for i in range(copies.shape[0]):
        copies[i, 0:16] = total
        copies[i, 16:24] = z_both[...]


def keep_kernel(array, kept):
    kept[...] = array[...]


def signal_kernel(got, weights, out):
    blocks = jnp.zeros((got.shape[0], weights.shape[2]), F32)
    faces = weights.shape[1]
    for q in range(weights.shape[0]):
        for c in range(3):
            width = min(128, faces - 128 * c)
            data = got[:, 3 * q + c, 0:width].astype(BF16)
            blocks = blocks + jnp.dot(data, weights[q, 128 * c : 128 * c + width, :], preferred_element_type=F32)
    total = jnp.sum(blocks, axis=0, keepdims=True)
    size = out.shape[2]
    for g in range(out.shape[0]):
        out[g] = total[:, g * size : (g + 1) * size]


def sum_kernel(tiles, out):
    total = tiles[0]
    for g in range(1, tiles.shape[0]):
        total = total + tiles[g]
    out[...] = total


def call(kernel, outs, args, scratch=(), flops=1_000_000, hbm=(), limit=16, aliases=None):
    single = not isinstance(outs, (list, tuple))
    inside = pl.BlockSpec(memory_space=pltpu.VMEM)
    return pl.pallas_call(
        kernel,
        out_shape=outs,
        in_specs=[pl.BlockSpec(memory_space=pltpu.HBM) if i in hbm else inside for i in range(len(args))],
        out_specs=inside if single else [inside] * len(outs),
        scratch_shapes=scratch,
        input_output_aliases=aliases or {},
        compiler_params=pltpu.CompilerParams(vmem_limit_bytes=limit * 1024 * 1024),
        cost_estimate=pl.CostEstimate(flops=flops, bytes_accessed=200_000, transcendentals=0),
    )(*args)


def step(density, velocity, pressure, blending, face_signal_weights, surf_id, surface_face_code):
    nx, ny, nz = density.shape
    sds = jax.ShapeDtypeStruct
    groups = lax.axis_size("gx") * lax.axis_size("gy")
    layers = lax.axis_size("gz")
    _, faces, local = face_signal_weights.shape
    ids = surf_id.reshape(1, -1)
    codes = surface_face_code.reshape(1, -1)
    slots = ids.shape[1]
    speeds = jnp.transpose(velocity, (1, 2, 0, 3))
    blocks, x_lo, x_hi, y_lo, y_hi, z_both, grid = call(
        functools.partial(face_kernel, faces),
        [sds((groups, 16, 128), BF16)]
        + [sds((5, ny, nz), F32)] * 2
        + [sds((5, nx, nz), F32)] * 2
        + [sds((8, 128), F32), sds((5, nx, 8, LANES), F32)],
        [density, speeds, pressure, ids, codes],
        [
            pltpu.VMEM((32, nz), F32),
            pltpu.VMEM((nx, ny, nz), F32),
            pltpu.VMEM((nx, ny, 3, nz), F32),
            pltpu.VMEM((nx, ny, nz), F32),
            pltpu.VMEM((1, slots), jnp.int32),
            pltpu.VMEM((1, slots), jnp.int32),
            pltpu.SemaphoreType.DMA((5,)),
        ],
        hbm=(0, 1, 2, 3, 4),
        limit=60,
    )
    arrived = lax.all_to_all(blocks, PAIR, 0, 0, tiled=True)
    held = call(
        keep_kernel, sds(face_signal_weights.shape, BF16), [face_signal_weights], flops=2_000_000
    )
    z_kept = call(keep_kernel, sds(z_both.shape, F32), [z_both])

    def shift(array, axis, step):
        peers = lax.axis_size(axis)
        return lax.ppermute(array, axis, [(i, (i + step) % peers) for i in range(peers)])

    x_low = shift(x_hi, "gx", 1)
    x_up = shift(x_lo, "gx", -1)
    y_low = shift(y_hi, "gy", 1)
    y_up = shift(y_lo, "gy", -1)

    copies = call(gather_kernel, sds((layers, 24, 128), F32), [arrived, z_kept])
    everywhere = lax.all_to_all(copies, "gz", 0, 0, tiled=True)
    partial = call(signal_kernel, sds((groups, 1, local // groups), F32), [everywhere, held])
    tiles = lax.all_to_all(partial, PAIR, 0, 0, tiled=True)
    signals = call(sum_kernel, sds((1, local // groups), F32), [tiles]).reshape(-1)

    tendency = call(
        tendency_kernel,
        sds((5, nx, ny, nz), F32),
        [grid, blending.reshape(1, -1), x_low, x_up, y_low, y_up, everywhere],
        [pltpu.VMEM((5, nx + 2, 8, LANES), F32)],
        flops=20_000_000,
    )
    return (tendency, signals)


def solution(mesh):
    placed = (
        P("gx", "gy", "gz"),
        P(None, "gx", "gy", "gz"),
        P("gx", "gy", "gz"),
        P("gx", "gy", "gz"),
        P(None, ("gx", "gy"), "gz"),
        P(("gx", "gy", "gz")),
        P(("gx", "gy", "gz")),
    )
    return jax.shard_map(
        step,
        mesh=mesh,
        in_specs=placed,
        out_specs=(P(None, "gx", "gy", "gz"), P(("gz", "gx", "gy"))),
        check_vma=False,
    )
```

```python
import functools
import math

import jax
import jax.numpy as jnp
import numpy as np
from jax import lax
from jax.experimental import pallas as pl
from jax.experimental.pallas import tpu as pltpu
from jax.sharding import PartitionSpec as P


GAMMA = 1.4
NODES = 5
PAIR = ("gx", "gy")
PLACE_FIRST = 21
SHARE_FIRST = 4
COLLECT_FIRST = 17


def rotated(count, first):
    return [(i + first) % count for i in range(count)]


LANES = 256
F32 = jnp.float32
BF16 = jnp.bfloat16


def gauss_lobatto():
    inner_root = math.sqrt(3.0 / 7.0)
    points = np.array([-1.0, -inner_root, 0.0, inner_root, 1.0])
    quad_weights = np.array([0.1, 49.0 / 90.0, 32.0 / 45.0, 49.0 / 90.0, 0.1])
    barycentric = np.ones(5)
    for target in range(5):
        for source in range(5):
            if source != target:
                barycentric[target] = barycentric[target] / (points[target] - points[source])
    derivative = np.zeros((5, 5))
    for target in range(5):
        for source in range(5):
            if source != target:
                derivative[target, source] = (
                    barycentric[source] / barycentric[target] / (points[target] - points[source])
                )
        derivative[target, target] = -np.sum(derivative[target])
    return (derivative, quad_weights)


DERIV, WEIGHTS = gauss_lobatto()


def iota(shape, dim):
    return lax.broadcasted_iota(jnp.int32, shape, dim)


def by_node(node, values):
    picked = jnp.zeros(node.shape, F32)
    for n, value in enumerate(values):
        if value != 0.0:
            picked = jnp.where(node == n, F32(value), picked)
    return picked


def flux4(rho, vel, pressure, d):
    mass = rho * vel[d]
    return [mass] + [mass * vel[m] + pressure if m == d else mass * vel[m] for m in range(3)]


def lay_out(den, vel, pre, grid):
    nx, ny, nz = den.shape
    for x in range(nx):
        grid[0, x, 0:ny, 0:nz] = den[x]
        grid[4, x, 0:ny, 0:nz] = pre[x]
        for y in range(ny):
            for m in range(3):
                grid[1 + m, x, y : y + 1, 0:nz] = vel[x, y, m : m + 1, :]


def face_kernel(per_group, den, vel, pre, sid, code, blocks, x_lo, x_hi, y_lo, y_hi, z_both, grid, rows, den_v, vel_v, pre_v, sid_v, code_v, sems):
    pairs = ((den, den_v), (vel, vel_v), (pre, pre_v), (sid, sid_v), (code, code_v))
    loads = [pltpu.make_async_copy(src, dst, sems.at[i]) for i, (src, dst) in enumerate(pairs)]
    for load in loads:
        load.start()
    nx, ny, nz = den.shape
    slots = sid.shape[1]
    groups = blocks.shape[0]
    rows[...] = jnp.zeros_like(rows)
    for load in loads:
        load.wait()

    lay_out(den_v, vel_v, pre_v, grid)

    def field(f, x):
        return grid[f, x, 0:ny, 0:nz]

    wy = by_node(iota((ny, nz), 0), WEIGHTS)

    sum_y = [None] * 4
    sum_z = [None] * 4
    for x in range(nx):
        rho, v, p = field(0, x), [field(1 + m, x) for m in range(3)], field(4, x)
        for q, value in enumerate(flux4(rho, v, p, 1)):
            term = F32(WEIGHTS[x]) * value
            sum_y[q] = term if sum_y[q] is None else sum_y[q] + term
        for q, value in enumerate(flux4(rho, v, p, 2)):
            term = F32(WEIGHTS[x]) * value
            sum_z[q] = term if sum_z[q] is None else sum_z[q] + term
        if x in (0, nx - 1):
            side, sign = (0, -1.0) if x == 0 else (1, 1.0)
            for q, value in enumerate(flux4(rho, v, p, 0)):
                rows[8 * q + side : 8 * q + side + 1, :] = F32(sign) * jnp.sum(wy * value, axis=0, keepdims=True)
    for q in range(4):
        rows[8 * q + 2 : 8 * q + 3, :] = -sum_y[q][0:1]
        rows[8 * q + 3 : 8 * q + 4, :] = sum_y[q][ny - 1 : ny]
        over_z = jnp.sum(wy * sum_z[q], axis=0, keepdims=True)
        rows[8 * q + 4 : 8 * q + 5, :] = -over_z
        rows[8 * q + 5 : 8 * q + 6, :] = over_z

    face = lax.shift_right_logical(code_v[...], 5)
    elem = code_v[...] & 31
    z = iota((nz, slots), 0)
    z_elem = lax.shift_right_logical(z * 52429, 18)
    z_node = z - 5 * z_elem
    plane = jnp.where(z_node == 4 * (face - 4), F32(1), F32(0))
    pick = jnp.where(z_elem == elem, jnp.where(face < 4, by_node(z_node, WEIGHTS), plane), F32(0))
    by_face = jnp.dot(rows[...], pick, precision=lax.Precision.HIGHEST, preferred_element_type=F32)
    face_hot = iota((8, slots), 0) == face
    data = [
        jnp.sum(jnp.where(face_hot, by_face[8 * q : 8 * q + 8], F32(0)), axis=0, keepdims=True)
        for q in range(4)
    ]

    ids = sid_v[...]
    group = lax.shift_right_logical(jnp.maximum(ids, 0) * 6554, 21)
    offset = ids - per_group * group
    chunk = lax.shift_right_logical(jnp.maximum(offset, 0), 7)
    group = jnp.where(ids >= 0, (group + groups - PLACE_FIRST) & (groups - 1), -1)
    row = iota((16, slots), 0)
    row_q = lax.shift_right_logical(row * 21846, 16)
    spread = jnp.zeros((16, slots), F32)
    for q in range(4):
        spread = jnp.where(row_q == q, data[q], spread)
    spread = jnp.where(row - 3 * row_q == chunk, spread, F32(0)).astype(BF16).astype(F32)
    group_of = iota((groups, 16, slots), 0)
    spread = jnp.where(group_of == group[None], spread[None], F32(0))
    spread = spread.reshape(groups * 16, slots).astype(BF16)
    lane_hot = (iota((128, slots), 0) == (offset & 127)).astype(F32).astype(BF16)
    placed = lax.dot_general(spread, lane_hot, (((1,), (1,)), ((), ())), preferred_element_type=F32)
    blocks[...] = placed.astype(BF16).reshape(groups, 16, 128)

    for f in range(5):
        x_lo[f] = grid[f, 0, 0:ny, 0:nz]
        x_hi[f] = grid[f, nx - 1, 0:ny, 0:nz]
        for x in range(nx):
            y_lo[f, x : x + 1] = grid[f, x, 0:1, 0:nz]
            y_hi[f, x : x + 1] = grid[f, x, ny - 1 : ny, 0:nz]

    z_both[...] = jnp.zeros_like(z_both)
    packed = jnp.zeros((ny, 128), F32)
    lane = iota((ny, 128), 1)
    for f in range(5):
        for x in range(nx):
            at = 5 * f + x
            packed = jnp.where(lane == at, grid[f, x, 0:ny, 0:1], packed)
            packed = jnp.where(lane == 64 + at, grid[f, x, 0:ny, nz - 1 : nz], packed)
    z_both[0:ny] = packed


def split_flux(a, b, d):
    half = [F32(0.5) * (x + y) for x, y in zip(a, b)]
    rho, vel, pressure, specific = half[0], half[1:4], half[4], half[5]
    mass = rho * vel[d]
    out = [mass]
    for m in range(3):
        value = mass * vel[m]
        out.append(value + pressure if m == d else value)
    out.append(mass * specific + pressure * vel[d])
    return out


def node_parts(a, d):
    rho, vel, pressure, specific, sound = a[0], a[1:4], a[4], a[5], a[6]
    cons = [rho] + [rho * v for v in vel] + [rho * specific]
    mass = cons[1 + d]
    flux = [mass] + [mass * vel[m] + pressure if m == d else mass * vel[m] for m in range(3)]
    flux.append((cons[4] + pressure) * vel[d])
    return flux, cons, jnp.abs(vel[d]) + sound


def rusanov(left, right):
    speed = F32(0.5) * jnp.maximum(left[2], right[2])
    return [
        F32(0.5) * (fl + fr) - speed * (ur - ul)
        for fl, fr, ul, ur in zip(left[0], right[0], left[1], right[1])
    ]


def derived(rho, v1, v2, v3, pressure):
    inverse = F32(1) / rho
    ratio = pressure * inverse
    specific = ratio * F32(1.0 / (GAMMA - 1.0)) + F32(0.5) * (v1 * v1 + v2 * v2 + v3 * v3)
    return [rho, v1, v2, v3, pressure, specific, jnp.sqrt(F32(GAMMA) * ratio)]


def tendency_kernel(start, blend, x_low, x_up, y_low, y_up, z_all, out, grid):
    _, nx, ny, nz = out.shape
    shape = (8, LANES)
    grid[...] = jnp.ones_like(grid)
    layers = z_all.shape[0]
    here = lax.axis_index("gz")
    at = here + 2 * layers - SHARE_FIRST
    z_low = z_all[lax.rem(at - 1, layers), 16:24]
    z_up = z_all[lax.rem(at + 1, layers), 16:24]
    half_lane = iota((8, 128), 1)
    outside = (iota((8, 128), 0) >= ny) & (half_lane >= nz - 128)
    for f in range(5):
        grid[f, 0, 0:ny, 0:nz] = x_low[f]
        grid[f, 1 + nx, 0:ny, 0:nz] = x_up[f]
        for x in range(nx):
            grid[f, 1 + x, 0:ny, 0:nz] = start[f, x, 0:ny, 0:nz]
            grid[f, 1 + x, ny : ny + 1, 0:nz] = y_up[f, x : x + 1]
            grid[f, 1 + x, 7:8, 0:nz] = y_low[f, x : x + 1]
            at = 5 * f + x
            upper = grid[f, 1 + x, :, 128:256]
            upper = jnp.where(half_lane == nz - 128, pltpu.roll(z_up, (nz - 128 - at) % 128, 1), upper)
            upper = jnp.where(half_lane == 127, pltpu.roll(z_low, (127 - 64 - at) % 128, 1), upper)
            upper = jnp.where(outside, F32(1), upper)
            grid[f, 1 + x, :, 128:256] = upper

    def state(x):
        return derived(*[grid[f, 1 + x] for f in range(5)])

    row = iota(shape, 0)
    lane = iota(shape, 1)
    lane_elem = lax.shift_right_logical(lane * 52429, 18)
    node = lane - 5 * lane_elem
    elems = blend.shape[1]
    spread = (iota((elems, LANES), 0) == lax.shift_right_logical(iota((elems, LANES), 1) * 52429, 18)).astype(F32)
    alpha = jnp.dot(
        jnp.broadcast_to(blend[...], (8, elems)), spread, precision=lax.Precision.HIGHEST, preferred_element_type=F32
    )
    keep = F32(1) - alpha
    inv = 1.0 / WEIGHTS

    def sides(index):
        inverse = by_node(index, inv)
        up = inverse * jnp.where(index == NODES - 1, F32(1), alpha)
        low = inverse * jnp.where(index == 0, F32(1), alpha)
        return up, low

    def pair_factors(index):
        ups = [by_node(index, [2.0 * DERIV[i, i + k] if i + k < NODES else 0.0 for i in range(NODES)]) for k in range(1, NODES)]
        downs = [by_node(index, [2.0 * DERIV[i, i - k] if i >= k else 0.0 for i in range(NODES)]) for k in range(1, NODES)]
        return ups, downs

    states = [state(x) for x in range(-1, nx + 1)]
    parts = [node_parts(s, 0) for s in states]
    faces = [rusanov(parts[i], parts[i + 1]) for i in range(nx + 1)]
    high = [[None] * 5 for _ in range(nx)]
    for i in range(nx):
        for j in range(i + 1, nx):
            pair = split_flux(states[1 + i], states[1 + j], 0)
            for c in range(5):
                for target, source in ((i, j), (j, i)):
                    term = F32(2.0 * DERIV[target, source]) * pair[c]
                    high[target][c] = term if high[target][c] is None else high[target][c] + term
    total = [[None] * 5 for _ in range(nx)]
    for x in range(nx):
        up = F32(inv[x]) if x == nx - 1 else F32(inv[x]) * alpha
        low = F32(inv[x]) if x == 0 else F32(inv[x]) * alpha
        for c in range(5):
            total[x][c] = keep * high[x][c] + (up * faces[x + 1][c] - low * faces[x][c])

    for d, axis, size, index in ((1, 0, 8, row), (2, 1, LANES, node)):
        ups, downs = pair_factors(index)
        up, low = sides(index)
        for x in range(nx):
            node_here = states[1 + x]
            high_x = [None] * 5
            for k in range(1, NODES):
                there = [pltpu.roll(s, size - k, axis) for s in (node_here if k == 1 else node_here[:6])]
                pair = split_flux(node_here[:6], there[:6], d)
                for c in range(5):
                    term = ups[k - 1] * pair[c] + downs[k - 1] * pltpu.roll(pair[c], k, axis)
                    high_x[c] = term if high_x[c] is None else high_x[c] + term
                if k == 1:
                    face = rusanov(node_parts(node_here, d), node_parts(there, d))
                    edge = [up * f - low * pltpu.roll(f, 1, axis) for f in face]
            for c in range(5):
                total[x][c] = total[x][c] + (keep * high_x[c] + edge[c])
    for x in range(nx):
        for c in range(5):
            out[c, x] = (-total[x][c])[0:ny, 0:nz]


def gather_kernel(got, z_both, copies):
    total = got[0].astype(F32)
    for i in range(1, got.shape[0]):
        total = total + got[i].astype(F32)
    for i in range(copies.shape[0]):
        copies[i, 0:16] = total
        copies[i, 16:24] = z_both[...]


def keep_kernel(array, kept):
    kept[...] = array[...]


def signal_kernel(got, weights, out):
    blocks = jnp.zeros((got.shape[0], weights.shape[2]), F32)
    faces = weights.shape[1]
    for q in range(weights.shape[0]):
        for c in range(3):
            width = min(128, faces - 128 * c)
            data = got[:, 3 * q + c, 0:width].astype(BF16)
            blocks = blocks + jnp.dot(data, weights[q, 128 * c : 128 * c + width, :], preferred_element_type=F32)
    total = jnp.sum(blocks, axis=0, keepdims=True)
    size = out.shape[2]
    for g in range(out.shape[0]):
        at = (g + COLLECT_FIRST) % out.shape[0]
        out[g] = total[:, at * size : (at + 1) * size]


def sum_kernel(tiles, out):
    total = tiles[0]
    for g in range(1, tiles.shape[0]):
        total = total + tiles[g]
    out[...] = total


def call(kernel, outs, args, scratch=(), flops=1_000_000, hbm=(), limit=16, aliases=None):
    single = not isinstance(outs, (list, tuple))
    inside = pl.BlockSpec(memory_space=pltpu.VMEM)
    return pl.pallas_call(
        kernel,
        out_shape=outs,
        in_specs=[pl.BlockSpec(memory_space=pltpu.HBM) if i in hbm else inside for i in range(len(args))],
        out_specs=inside if single else [inside] * len(outs),
        scratch_shapes=scratch,
        input_output_aliases=aliases or {},
        compiler_params=pltpu.CompilerParams(vmem_limit_bytes=limit * 1024 * 1024),
        cost_estimate=pl.CostEstimate(flops=flops, bytes_accessed=200_000, transcendentals=0),
    )(*args)


def step(density, velocity, pressure, blending, face_signal_weights, surf_id, surface_face_code):
    nx, ny, nz = density.shape
    sds = jax.ShapeDtypeStruct
    groups = lax.axis_size("gx") * lax.axis_size("gy")
    layers = lax.axis_size("gz")
    _, faces, local = face_signal_weights.shape
    ids = surf_id.reshape(1, -1)
    codes = surface_face_code.reshape(1, -1)
    slots = ids.shape[1]
    speeds = jnp.transpose(velocity, (1, 2, 0, 3))
    blocks, x_lo, x_hi, y_lo, y_hi, z_both, grid = call(
        functools.partial(face_kernel, faces),
        [sds((groups, 16, 128), BF16)]
        + [sds((5, ny, nz), F32)] * 2
        + [sds((5, nx, nz), F32)] * 2
        + [sds((8, 128), F32), sds((5, nx, 8, LANES), F32)],
        [density, speeds, pressure, ids, codes],
        [
            pltpu.VMEM((32, nz), F32),
            pltpu.VMEM((nx, ny, nz), F32),
            pltpu.VMEM((nx, ny, 3, nz), F32),
            pltpu.VMEM((nx, ny, nz), F32),
            pltpu.VMEM((1, slots), jnp.int32),
            pltpu.VMEM((1, slots), jnp.int32),
            pltpu.SemaphoreType.DMA((5,)),
        ],
        hbm=(0, 1, 2, 3, 4),
        limit=60,
    )
    arrived = lax.all_to_all(blocks, PAIR, 0, 0, tiled=True, axis_index_groups=[rotated(groups, PLACE_FIRST)])
    held = call(
        keep_kernel, sds(face_signal_weights.shape, BF16), [face_signal_weights], flops=2_000_000
    )
    z_kept = call(keep_kernel, sds(z_both.shape, F32), [z_both])

    def shift(array, axis, step):
        peers = lax.axis_size(axis)
        return lax.ppermute(array, axis, [(i, (i + step) % peers) for i in range(peers)])

    x_low = shift(x_hi, "gx", 1)
    x_up = shift(x_lo, "gx", -1)
    y_low = shift(y_hi, "gy", 1)
    y_up = shift(y_lo, "gy", -1)

    copies = call(gather_kernel, sds((layers, 24, 128), F32), [arrived, z_kept])
    everywhere = lax.all_to_all(copies, "gz", 0, 0, tiled=True, axis_index_groups=[rotated(layers, SHARE_FIRST)])
    partial = call(signal_kernel, sds((groups, 1, local // groups), F32), [everywhere, held])
    tiles = lax.all_to_all(partial, PAIR, 0, 0, tiled=True, axis_index_groups=[rotated(groups, COLLECT_FIRST)])
    signals = call(sum_kernel, sds((1, local // groups), F32), [tiles]).reshape(-1)

    tendency = call(
        tendency_kernel,
        sds((5, nx, ny, nz), F32),
        [grid, blending.reshape(1, -1), x_low, x_up, y_low, y_up, everywhere],
        [pltpu.VMEM((5, nx + 2, 8, LANES), F32)],
        flops=20_000_000,
    )
    return (tendency, signals)


def solution(mesh):
    placed = (
        P("gx", "gy", "gz"),
        P(None, "gx", "gy", "gz"),
        P("gx", "gy", "gz"),
        P("gx", "gy", "gz"),
        P(None, ("gx", "gy"), "gz"),
        P(("gx", "gy", "gz")),
        P(("gx", "gy", "gz")),
    )
    return jax.shard_map(
        step,
        mesh=mesh,
        in_specs=placed,
        out_specs=(P(None, "gx", "gy", "gz"), P(("gz", "gx", "gy"))),
        check_vma=False,
    )
```

```python
import functools
import math

import jax
import jax.numpy as jnp
import numpy as np
from jax import lax
from jax.experimental import pallas as pl
from jax.experimental.pallas import tpu as pltpu
from jax.sharding import PartitionSpec as P


GAMMA = 1.4
NODES = 5
PAIR = ("gx", "gy")
PLACE_FIRST = 21
SHARE_FIRST = 4
COLLECT_FIRST = 17
Z_ROWS = 10
HINT_FLOPS = 20_000_000_000
HINT_BYTES = 800_000_000


def rotated(count, first):
    return [(i + first) % count for i in range(count)]


LANES = 256
F32 = jnp.float32
BF16 = jnp.bfloat16


def gauss_lobatto():
    inner_root = math.sqrt(3.0 / 7.0)
    points = np.array([-1.0, -inner_root, 0.0, inner_root, 1.0])
    quad_weights = np.array([0.1, 49.0 / 90.0, 32.0 / 45.0, 49.0 / 90.0, 0.1])
    barycentric = np.ones(5)
    for target in range(5):
        for source in range(5):
            if source != target:
                barycentric[target] = barycentric[target] / (points[target] - points[source])
    derivative = np.zeros((5, 5))
    for target in range(5):
        for source in range(5):
            if source != target:
                derivative[target, source] = (
                    barycentric[source] / barycentric[target] / (points[target] - points[source])
                )
        derivative[target, target] = -np.sum(derivative[target])
    return (derivative, quad_weights)


DERIV, WEIGHTS = gauss_lobatto()


def iota(shape, dim):
    return lax.broadcasted_iota(jnp.int32, shape, dim)


def by_node(node, values):
    picked = jnp.zeros(node.shape, F32)
    for n, value in enumerate(values):
        if value != 0.0:
            picked = jnp.where(node == n, F32(value), picked)
    return picked


def flux4(rho, vel, pressure, d):
    mass = rho * vel[d]
    return [mass] + [mass * vel[m] + pressure if m == d else mass * vel[m] for m in range(3)]


def lay_out(den, vel, pre, grid):
    nx, ny, nz = den.shape
    for x in range(nx):
        grid[0, x, 0:ny, 0:nz] = den[x]
        grid[4, x, 0:ny, 0:nz] = pre[x]
        for y in range(ny):
            for m in range(3):
                grid[1 + m, x, y : y + 1, 0:nz] = vel[x, y, m : m + 1, :]


def face_kernel(per_group, mask, den, vel, pre, sid, code, blocks, x_lo, x_hi, y_lo, y_hi, z_both, grid, rows):
    nx, ny, nz = den.shape
    slots = sid.shape[1]
    groups = blocks.shape[0]
    rows[...] = jnp.zeros_like(rows)
    lay_out(den, vel, pre, grid)

    def field(f, x):
        return grid[f, x, 0:ny, 0:nz]

    wy = by_node(iota((ny, nz), 0), WEIGHTS)

    sum_y = [None] * 4
    sum_z = [None] * 4
    for x in range(nx):
        rho, v, p = field(0, x), [field(1 + m, x) for m in range(3)], field(4, x)
        for q, value in enumerate(flux4(rho, v, p, 1)):
            term = F32(WEIGHTS[x]) * value
            sum_y[q] = term if sum_y[q] is None else sum_y[q] + term
        for q, value in enumerate(flux4(rho, v, p, 2)):
            term = F32(WEIGHTS[x]) * value
            sum_z[q] = term if sum_z[q] is None else sum_z[q] + term
        if x in (0, nx - 1):
            side, sign = (0, -1.0) if x == 0 else (1, 1.0)
            for q, value in enumerate(flux4(rho, v, p, 0)):
                rows[8 * q + side : 8 * q + side + 1, :] = F32(sign) * jnp.sum(wy * value, axis=0, keepdims=True)
    for q in range(4):
        rows[8 * q + 2 : 8 * q + 3, :] = -sum_y[q][0:1]
        rows[8 * q + 3 : 8 * q + 4, :] = sum_y[q][ny - 1 : ny]
        over_z = jnp.sum(wy * sum_z[q], axis=0, keepdims=True)
        rows[8 * q + 4 : 8 * q + 5, :] = -over_z
        rows[8 * q + 5 : 8 * q + 6, :] = over_z

    face = lax.shift_right_logical(code[...], 5)
    elem = code[...] & 31
    z = iota((nz, slots), 0)
    z_elem = lax.shift_right_logical(z * 52429, 18)
    z_node = z - 5 * z_elem
    plane = jnp.where(z_node == 4 * (face - 4), F32(1), F32(0))
    pick = jnp.where(z_elem == elem, jnp.where(face < 4, by_node(z_node, WEIGHTS), plane), F32(0))
    by_face = jnp.dot(rows[...], pick, precision=lax.Precision.HIGHEST, preferred_element_type=F32)
    face_hot = iota((8, slots), 0) == face
    data = [
        jnp.sum(jnp.where(face_hot, by_face[8 * q : 8 * q + 8], F32(0)), axis=0, keepdims=True)
        for q in range(4)
    ]

    ids = sid[...]
    group = lax.shift_right_logical(jnp.maximum(ids, 0) * 6554, 21)
    offset = ids - per_group * group
    group = jnp.where(ids >= 0, (group + groups - PLACE_FIRST) & (groups - 1), -1)
    row = iota((16, slots), 0)
    group_of = iota((groups, 16, slots), 0)
    placed = jnp.zeros((groups * 16, 128), F32)
    for shift in sorted({q * per_group % 128 for q in range(4)}):
        spread = jnp.zeros((16, slots), F32)
        for q in range(4):
            if q * per_group % 128 == shift:
                at = lax.shift_right_logical(jnp.maximum(q * per_group + offset, 0), 7)
                spread = jnp.where(row == at, data[q], spread)
        spread = spread.astype(BF16).astype(F32)
        spread = jnp.where(group_of == group[None], spread[None], F32(0))
        spread = spread.reshape(groups * 16, slots).astype(BF16)
        lane_hot = (iota((128, slots), 0) == ((shift + offset) & 127)).astype(F32).astype(BF16)
        placed += lax.dot_general(spread, lane_hot, (((1,), (1,)), ((), ())), preferred_element_type=F32)
    blocks[...] = placed.astype(BF16).reshape(groups, 16, 128)

    for f in range(5):
        x_lo[f] = grid[f, 0, 0:ny, 0:nz]
        x_hi[f] = grid[f, nx - 1, 0:ny, 0:nz]
        for x in range(nx):
            y_lo[f, x : x + 1] = grid[f, x, 0:1, 0:nz]
            y_hi[f, x : x + 1] = grid[f, x, ny - 1 : ny, 0:nz]

    z_both[...] = F32(1) - mask[...]
    z_both[0:Z_ROWS] = jnp.zeros((Z_ROWS, 128), F32)
    lane = iota((ny, 128), 1)
    for side, node in enumerate((0, nz - 1)):
        packed = jnp.zeros((ny, 128), F32)
        for f in range(5):
            for x in range(nx):
                packed = jnp.where(lane == nx * f + x, grid[f, x, 0:ny, node : node + 1], packed)
        rows[0:ny, 0:128] = packed
        rest = rows[0:1, 0:128]
        for y in range(1, ny):
            rest = rest + pltpu.roll(jnp.broadcast_to(rows[y : y + 1, 0:128], (8, 128)), 5 * nx * y, 1)[0:1]
        for part in range(3):
            rounded = rest.astype(BF16).astype(F32)
            z_both[Z_ROWS + 3 * side + part : Z_ROWS + 3 * side + part + 1] = rounded
            rest = rest - rounded


def split_flux(a, b, d):
    half = [F32(0.5) * (x + y) for x, y in zip(a, b)]
    rho, vel, pressure, specific = half[0], half[1:4], half[4], half[5]
    mass = rho * vel[d]
    out = [mass]
    for m in range(3):
        value = mass * vel[m]
        out.append(value + pressure if m == d else value)
    out.append(mass * specific + pressure * vel[d])
    return out


def node_parts(a, d):
    rho, vel, pressure, specific, sound = a[0], a[1:4], a[4], a[5], a[6]
    cons = [rho] + [rho * v for v in vel] + [rho * specific]
    mass = cons[1 + d]
    flux = [mass] + [mass * vel[m] + pressure if m == d else mass * vel[m] for m in range(3)]
    flux.append((cons[4] + pressure) * vel[d])
    return flux, cons, jnp.abs(vel[d]) + sound


def rusanov(left, right):
    speed = F32(0.5) * jnp.maximum(left[2], right[2])
    return [
        F32(0.5) * (fl + fr) - speed * (ur - ul)
        for fl, fr, ul, ur in zip(left[0], right[0], left[1], right[1])
    ]


def derived(rho, v1, v2, v3, pressure):
    inverse = F32(1) / rho
    ratio = pressure * inverse
    specific = ratio * F32(1.0 / (GAMMA - 1.0)) + F32(0.5) * (v1 * v1 + v2 * v2 + v3 * v3)
    return [rho, v1, v2, v3, pressure, specific, jnp.sqrt(F32(GAMMA) * ratio)]


def tendency_kernel(start, blend, x_low, x_up, y_low, y_up, z_all, out, grid):
    _, nx, ny, nz = out.shape
    shape = (8, LANES)
    grid[...] = jnp.ones_like(grid)
    layers = z_all.shape[0]
    here = lax.axis_index("gz")

    def from_layer(step, side):
        at = lax.rem(here + 2 * layers - SHARE_FIRST + step, layers)
        parts = z_all[at].astype(F32)
        first = Z_ROWS + 3 * side
        line = (parts[first + 2 : first + 3] + parts[first + 1 : first + 2]) + parts[first : first + 1]
        line = jnp.broadcast_to(line, (8, 128))
        found = line
        for y in range(1, ny):
            found = jnp.where(iota((8, 128), 0) == y, pltpu.roll(line, 128 - 5 * nx * y, 1), found)
        return found

    z_low = from_layer(-1, 1)
    z_up = from_layer(1, 0)
    half_lane = iota((8, 128), 1)
    outside = (iota((8, 128), 0) >= ny) & (half_lane >= nz - 128)
    for f in range(5):
        grid[f, 0, 0:ny, 0:nz] = x_low[f]
        grid[f, 1 + nx, 0:ny, 0:nz] = x_up[f]
        for x in range(nx):
            grid[f, 1 + x, 0:ny, 0:nz] = start[f, x, 0:ny, 0:nz]
            grid[f, 1 + x, ny : ny + 1, 0:nz] = y_up[f, x : x + 1]
            grid[f, 1 + x, 7:8, 0:nz] = y_low[f, x : x + 1]
            at = 5 * f + x
            upper = grid[f, 1 + x, :, 128:256]
            upper = jnp.where(half_lane == nz - 128, pltpu.roll(z_up, (nz - 128 - at) % 128, 1), upper)
            upper = jnp.where(half_lane == 127, pltpu.roll(z_low, (127 - at) % 128, 1), upper)
            upper = jnp.where(outside, F32(1), upper)
            grid[f, 1 + x, :, 128:256] = upper

    def state(x):
        return derived(*[grid[f, 1 + x] for f in range(5)])

    row = iota(shape, 0)
    lane = iota(shape, 1)
    lane_elem = lax.shift_right_logical(lane * 52429, 18)
    node = lane - 5 * lane_elem
    elems = blend.shape[1]
    spread = (iota((elems, LANES), 0) == lax.shift_right_logical(iota((elems, LANES), 1) * 52429, 18)).astype(F32)
    alpha = jnp.dot(
        jnp.broadcast_to(blend[...], (8, elems)), spread, precision=lax.Precision.HIGHEST, preferred_element_type=F32
    )
    keep = F32(1) - alpha
    inv = 1.0 / WEIGHTS

    def sides(index):
        inverse = by_node(index, inv)
        up = inverse * jnp.where(index == NODES - 1, F32(1), alpha)
        low = inverse * jnp.where(index == 0, F32(1), alpha)
        return up, low

    def pair_factors(index):
        ups = [by_node(index, [2.0 * DERIV[i, i + k] if i + k < NODES else 0.0 for i in range(NODES)]) for k in range(1, NODES)]
        downs = [by_node(index, [2.0 * DERIV[i, i - k] if i >= k else 0.0 for i in range(NODES)]) for k in range(1, NODES)]
        return ups, downs

    states = [state(x) for x in range(-1, nx + 1)]
    parts = [node_parts(s, 0) for s in states]
    faces = [rusanov(parts[i], parts[i + 1]) for i in range(nx + 1)]
    high = [[None] * 5 for _ in range(nx)]
    for i in range(nx):
        for j in range(i + 1, nx):
            pair = split_flux(states[1 + i], states[1 + j], 0)
            for c in range(5):
                for target, source in ((i, j), (j, i)):
                    term = F32(2.0 * DERIV[target, source]) * pair[c]
                    high[target][c] = term if high[target][c] is None else high[target][c] + term
    total = [[None] * 5 for _ in range(nx)]
    for x in range(nx):
        up = F32(inv[x]) if x == nx - 1 else F32(inv[x]) * alpha
        low = F32(inv[x]) if x == 0 else F32(inv[x]) * alpha
        for c in range(5):
            total[x][c] = keep * high[x][c] + (up * faces[x + 1][c] - low * faces[x][c])

    for d, axis, size, index in ((1, 0, 8, row), (2, 1, LANES, node)):
        ups, downs = pair_factors(index)
        up, low = sides(index)
        for x in range(nx):
            node_here = states[1 + x]
            high_x = [None] * 5
            for k in range(1, NODES):
                there = [pltpu.roll(s, size - k, axis) for s in (node_here if k == 1 else node_here[:6])]
                pair = split_flux(node_here[:6], there[:6], d)
                for c in range(5):
                    term = ups[k - 1] * pair[c] + downs[k - 1] * pltpu.roll(pair[c], k, axis)
                    high_x[c] = term if high_x[c] is None else high_x[c] + term
                if k == 1:
                    face = rusanov(node_parts(node_here, d), node_parts(there, d))
                    edge = [up * f - low * pltpu.roll(f, 1, axis) for f in face]
            for c in range(5):
                total[x][c] = total[x][c] + (keep * high_x[c] + edge[c])
    for x in range(nx):
        for c in range(5):
            out[c, x] = (-total[x][c])[0:ny, 0:nz]


def gather_kernel(got, z_both, copies):
    total = z_both[...]
    for i in range(got.shape[0]):
        total = total + got[i].astype(F32)
    total = total.astype(BF16)
    for i in range(copies.shape[0]):
        copies[i] = total


def mask_kernel(mask):
    mask[...] = jnp.where(iota(mask.shape, 0) >= Z_ROWS, F32(1), F32(0))


def signal_kernel(got, weights, out):
    data = got[0].astype(F32)
    for i in range(1, got.shape[0]):
        data = data + got[i].astype(F32)
    data = data.astype(BF16)
    total = jnp.zeros((1, weights.shape[2]), F32)
    faces = weights.shape[1]
    for q in range(weights.shape[0]):
        face = 0
        while face < faces:
            row, lane = divmod(q * faces + face, 128)
            width = min(128 - lane, faces - face)
            part = data[row : row + 1, lane : lane + width]
            total = total + jnp.dot(part, weights[q, face : face + width, :], preferred_element_type=F32)
            face += width
    size = out.shape[2]
    for g in range(out.shape[0]):
        at = (g + COLLECT_FIRST) % out.shape[0]
        out[g] = total[:, at * size : (at + 1) * size]


def sum_kernel(tiles, out):
    total = tiles[0]
    for g in range(1, tiles.shape[0]):
        total = total + tiles[g]
    out[...] = total


def call(kernel, outs, args, scratch=(), flops=1_000_000, hbm=(), limit=16, aliases=None, moved=200_000):
    single = not isinstance(outs, (list, tuple))
    inside = pl.BlockSpec(memory_space=pltpu.VMEM)
    return pl.pallas_call(
        kernel,
        out_shape=outs,
        in_specs=[pl.BlockSpec(memory_space=pltpu.HBM) if i in hbm else inside for i in range(len(args))],
        out_specs=inside if single else [inside] * len(outs),
        scratch_shapes=scratch,
        input_output_aliases=aliases or {},
        compiler_params=pltpu.CompilerParams(vmem_limit_bytes=limit * 1024 * 1024),
        cost_estimate=pl.CostEstimate(flops=flops, bytes_accessed=moved, transcendentals=0),
    )(*args)


def step(density, velocity, pressure, blending, face_signal_weights, surf_id, surface_face_code):
    nx, ny, nz = density.shape
    sds = jax.ShapeDtypeStruct
    groups = lax.axis_size("gx") * lax.axis_size("gy")
    layers = lax.axis_size("gz")
    _, faces, local = face_signal_weights.shape
    ids = surf_id.reshape(1, -1)
    codes = surface_face_code.reshape(1, -1)
    speeds = jnp.transpose(velocity, (1, 2, 0, 3))
    mask = call(mask_kernel, sds((16, 128), F32), [], flops=HINT_FLOPS, moved=HINT_BYTES)
    blocks, x_lo, x_hi, y_lo, y_hi, z_both, grid = call(
        functools.partial(face_kernel, faces),
        [sds((groups, 16, 128), BF16)]
        + [sds((5, ny, nz), F32)] * 2
        + [sds((5, nx, nz), F32)] * 2
        + [sds((16, 128), F32), sds((5, nx, 8, LANES), F32)],
        [mask, density, speeds, pressure, ids, codes],
        [
            pltpu.VMEM((32, nz), F32),
        ],
    )
    arrived = lax.all_to_all(blocks, PAIR, 0, 0, tiled=True, axis_index_groups=[rotated(groups, PLACE_FIRST)])

    def shift(array, axis, step):
        peers = lax.axis_size(axis)
        return lax.ppermute(array, axis, [(i, (i + step) % peers) for i in range(peers)])

    x_low = shift(x_hi, "gx", 1)
    x_up = shift(x_lo, "gx", -1)
    y_low = shift(y_hi, "gy", 1)
    y_up = shift(y_lo, "gy", -1)

    copies = call(gather_kernel, sds((layers, 16, 128), BF16), [arrived, z_both], flops=HINT_FLOPS, moved=HINT_BYTES)
    everywhere = lax.all_to_all(copies, "gz", 0, 0, tiled=True, axis_index_groups=[rotated(layers, SHARE_FIRST)])
    partial = call(signal_kernel, sds((groups, 1, local // groups), F32), [everywhere, face_signal_weights])
    tiles = lax.all_to_all(partial, PAIR, 0, 0, tiled=True, axis_index_groups=[rotated(groups, COLLECT_FIRST)])
    signals = call(sum_kernel, sds((1, local // groups), F32), [tiles]).reshape(-1)

    tendency = call(
        tendency_kernel,
        sds((5, nx, ny, nz), F32),
        [grid, blending.reshape(1, -1), x_low, x_up, y_low, y_up, everywhere],
        [pltpu.VMEM((5, nx + 2, 8, LANES), F32)],
        flops=20_000_000,
    )
    return (tendency, signals)


def solution(mesh):
    placed = (
        P("gx", "gy", "gz"),
        P(None, "gx", "gy", "gz"),
        P("gx", "gy", "gz"),
        P("gx", "gy", "gz"),
        P(None, ("gx", "gy"), "gz"),
        P(("gx", "gy", "gz")),
        P(("gx", "gy", "gz")),
    )
    return jax.shard_map(
        step,
        mesh=mesh,
        in_specs=placed,
        out_specs=(P(None, "gx", "gy", "gz"), P(("gz", "gx", "gy"))),
        check_vma=False,
    )
```

```python
import functools
import math

import jax
import jax.numpy as jnp
import numpy as np
from jax import lax
from jax.experimental import pallas as pl
from jax.experimental.pallas import tpu as pltpu
from jax.sharding import PartitionSpec as P


GAMMA = 1.4
NODES = 5
PAIR = ("gx", "gy")
PLACE_FIRST = 21
SHARE_FIRST = 4
COLLECT_FIRST = 21
Z_ROWS = 10
HINT_FLOPS = 20_000_000_000
HINT_BYTES = 800_000_000


def rotated(count, first):
    return [(i + first) % count for i in range(count)]


LANES = 256
F32 = jnp.float32
BF16 = jnp.bfloat16


def gauss_lobatto():
    inner_root = math.sqrt(3.0 / 7.0)
    points = np.array([-1.0, -inner_root, 0.0, inner_root, 1.0])
    quad_weights = np.array([0.1, 49.0 / 90.0, 32.0 / 45.0, 49.0 / 90.0, 0.1])
    barycentric = np.ones(5)
    for target in range(5):
        for source in range(5):
            if source != target:
                barycentric[target] = barycentric[target] / (points[target] - points[source])
    derivative = np.zeros((5, 5))
    for target in range(5):
        for source in range(5):
            if source != target:
                derivative[target, source] = (
                    barycentric[source] / barycentric[target] / (points[target] - points[source])
                )
        derivative[target, target] = -np.sum(derivative[target])
    return (derivative, quad_weights)


DERIV, WEIGHTS = gauss_lobatto()


def iota(shape, dim):
    return lax.broadcasted_iota(jnp.int32, shape, dim)


def by_node(node, values):
    picked = jnp.zeros(node.shape, F32)
    for n, value in enumerate(values):
        if value != 0.0:
            picked = jnp.where(node == n, F32(value), picked)
    return picked


def is_even(axis, shape):
    return (jnp.zeros(shape, jnp.int32) + lax.axis_index(axis)) & 1 == 0


def flux4(rho, vel, pressure, d):
    mass = rho * vel[d]
    return [mass] + [mass * vel[m] + pressure if m == d else mass * vel[m] for m in range(3)]


def lay_out(den, vel, pre, grid):
    nx, ny, nz = den.shape
    for x in range(nx):
        grid[0, x, 0:ny, 0:nz] = den[x]
        grid[4, x, 0:ny, 0:nz] = pre[x]
        for y in range(ny):
            for m in range(3):
                grid[1 + m, x, y : y + 1, 0:nz] = vel[x, y, m : m + 1, :]


def face_kernel(per_group, mask, den, vel, pre, sid, code, blocks, x_one, x_two, y_one, y_two, z_both, grid, rows):
    nx, ny, nz = den.shape
    slots = sid.shape[1]
    groups = blocks.shape[0]
    rows[...] = jnp.zeros_like(rows)
    lay_out(den, vel, pre, grid)

    def field(f, x):
        return grid[f, x, 0:ny, 0:nz]

    wy = by_node(iota((ny, nz), 0), WEIGHTS)

    sum_y = [None] * 4
    sum_z = [None] * 4
    for x in range(nx):
        rho, v, p = field(0, x), [field(1 + m, x) for m in range(3)], field(4, x)
        for q, value in enumerate(flux4(rho, v, p, 1)):
            term = F32(WEIGHTS[x]) * value
            sum_y[q] = term if sum_y[q] is None else sum_y[q] + term
        for q, value in enumerate(flux4(rho, v, p, 2)):
            term = F32(WEIGHTS[x]) * value
            sum_z[q] = term if sum_z[q] is None else sum_z[q] + term
        if x in (0, nx - 1):
            side, sign = (0, -1.0) if x == 0 else (1, 1.0)
            for q, value in enumerate(flux4(rho, v, p, 0)):
                rows[8 * q + side : 8 * q + side + 1, :] = F32(sign) * jnp.sum(wy * value, axis=0, keepdims=True)
    for q in range(4):
        rows[8 * q + 2 : 8 * q + 3, :] = -sum_y[q][0:1]
        rows[8 * q + 3 : 8 * q + 4, :] = sum_y[q][ny - 1 : ny]
        over_z = jnp.sum(wy * sum_z[q], axis=0, keepdims=True)
        rows[8 * q + 4 : 8 * q + 5, :] = -over_z
        rows[8 * q + 5 : 8 * q + 6, :] = over_z

    face = lax.shift_right_logical(code[...], 5)
    elem = code[...] & 31
    z = iota((nz, slots), 0)
    z_elem = lax.shift_right_logical(z * 52429, 18)
    z_node = z - 5 * z_elem
    plane = jnp.where(z_node == 4 * (face - 4), F32(1), F32(0))
    pick = jnp.where(z_elem == elem, jnp.where(face < 4, by_node(z_node, WEIGHTS), plane), F32(0))
    by_face = jnp.dot(rows[...], pick, precision=lax.Precision.HIGHEST, preferred_element_type=F32)
    face_hot = iota((8, slots), 0) == face
    data = [
        jnp.sum(jnp.where(face_hot, by_face[8 * q : 8 * q + 8], F32(0)), axis=0, keepdims=True)
        for q in range(4)
    ]

    ids = sid[...]
    group = lax.shift_right_logical(jnp.maximum(ids, 0) * 6554, 21)
    offset = ids - per_group * group
    group = jnp.where(ids >= 0, (group + groups - PLACE_FIRST) & (groups - 1), -1)
    row = iota((16, slots), 0)
    group_of = iota((groups, 16, slots), 0)
    placed = jnp.zeros((groups * 16, 128), F32)
    for shift in sorted({q * per_group % 128 for q in range(4)}):
        spread = jnp.zeros((16, slots), F32)
        for q in range(4):
            if q * per_group % 128 == shift:
                at = lax.shift_right_logical(jnp.maximum(q * per_group + offset, 0), 7)
                spread = jnp.where(row == at, data[q], spread)
        spread = spread.astype(BF16).astype(F32)
        spread = jnp.where(group_of == group[None], spread[None], F32(0))
        spread = spread.reshape(groups * 16, slots).astype(BF16)
        lane_hot = (iota((128, slots), 0) == ((shift + offset) & 127)).astype(F32).astype(BF16)
        placed += lax.dot_general(spread, lane_hot, (((1,), (1,)), ((), ())), preferred_element_type=F32)
    blocks[...] = placed.astype(BF16).reshape(groups, 16, 128)

    even_x, even_y = is_even("gx", (ny, nz)), is_even("gy", (1, nz))
    for f in range(5):
        low, high = field(f, 0), field(f, nx - 1)
        x_one[f] = jnp.where(even_x, high, low)
        x_two[f] = jnp.where(even_x, low, high)
        for x in range(nx):
            low, high = grid[f, x, 0:1, 0:nz], grid[f, x, ny - 1 : ny, 0:nz]
            y_one[f, x : x + 1] = jnp.where(even_y, high, low)
            y_two[f, x : x + 1] = jnp.where(even_y, low, high)

    z_both[...] = F32(1) - mask[...]
    z_both[0:Z_ROWS] = jnp.zeros((Z_ROWS, 128), F32)
    lane = iota((ny, 128), 1)
    for side, node in enumerate((0, nz - 1)):
        packed = jnp.zeros((ny, 128), F32)
        for f in range(5):
            for x in range(nx):
                packed = jnp.where(lane == nx * f + x, grid[f, x, 0:ny, node : node + 1], packed)
        rows[0:ny, 0:128] = packed
        rest = rows[0:1, 0:128]
        for y in range(1, ny):
            rest = rest + pltpu.roll(jnp.broadcast_to(rows[y : y + 1, 0:128], (8, 128)), 5 * nx * y, 1)[0:1]
        for part in range(3):
            rounded = rest.astype(BF16).astype(F32)
            z_both[Z_ROWS + 3 * side + part : Z_ROWS + 3 * side + part + 1] = rounded
            rest = rest - rounded


def split_flux(a, b, d):
    half = [F32(0.5) * (x + y) for x, y in zip(a, b)]
    rho, vel, pressure, specific = half[0], half[1:4], half[4], half[5]
    mass = rho * vel[d]
    out = [mass]
    for m in range(3):
        value = mass * vel[m]
        out.append(value + pressure if m == d else value)
    out.append(mass * specific + pressure * vel[d])
    return out


def node_parts(a, d):
    rho, vel, pressure, specific, sound = a[0], a[1:4], a[4], a[5], a[6]
    cons = [rho] + [rho * v for v in vel] + [rho * specific]
    mass = cons[1 + d]
    flux = [mass] + [mass * vel[m] + pressure if m == d else mass * vel[m] for m in range(3)]
    flux.append((cons[4] + pressure) * vel[d])
    return flux, cons, jnp.abs(vel[d]) + sound


def rusanov(left, right):
    speed = F32(0.5) * jnp.maximum(left[2], right[2])
    return [
        F32(0.5) * (fl + fr) - speed * (ur - ul)
        for fl, fr, ul, ur in zip(left[0], right[0], left[1], right[1])
    ]


def derived(rho, v1, v2, v3, pressure):
    inverse = F32(1) / rho
    ratio = pressure * inverse
    specific = ratio * F32(1.0 / (GAMMA - 1.0)) + F32(0.5) * (v1 * v1 + v2 * v2 + v3 * v3)
    return [rho, v1, v2, v3, pressure, specific, jnp.sqrt(F32(GAMMA) * ratio)]


def tendency_kernel(start, blend, x_one, x_two, y_one, y_two, z_all, out, grid):
    _, nx, ny, nz = out.shape
    shape = (8, LANES)
    grid[...] = jnp.ones_like(grid)
    layers = z_all.shape[0]
    here = lax.axis_index("gz")

    def from_layer(step, side):
        at = lax.rem(here + 2 * layers - SHARE_FIRST + step, layers)
        parts = z_all[at].astype(F32)
        first = Z_ROWS + 3 * side
        line = (parts[first + 2 : first + 3] + parts[first + 1 : first + 2]) + parts[first : first + 1]
        line = jnp.broadcast_to(line, (8, 128))
        found = line
        for y in range(1, ny):
            found = jnp.where(iota((8, 128), 0) == y, pltpu.roll(line, 128 - 5 * nx * y, 1), found)
        return found

    z_low = from_layer(-1, 1)
    z_up = from_layer(1, 0)
    even_x, even_y = is_even("gx", (ny, nz)), is_even("gy", (1, nz))
    half_lane = iota((8, 128), 1)
    outside = (iota((8, 128), 0) >= ny) & (half_lane >= nz - 128)
    for f in range(5):
        grid[f, 0, 0:ny, 0:nz] = jnp.where(even_x, x_two[f], x_one[f])
        grid[f, 1 + nx, 0:ny, 0:nz] = jnp.where(even_x, x_one[f], x_two[f])
        for x in range(nx):
            grid[f, 1 + x, 0:ny, 0:nz] = start[f, x, 0:ny, 0:nz]
            one, two = y_one[f, x : x + 1], y_two[f, x : x + 1]
            grid[f, 1 + x, ny : ny + 1, 0:nz] = jnp.where(even_y, one, two)
            grid[f, 1 + x, 7:8, 0:nz] = jnp.where(even_y, two, one)
            at = 5 * f + x
            upper = grid[f, 1 + x, :, 128:256]
            upper = jnp.where(half_lane == nz - 128, pltpu.roll(z_up, (nz - 128 - at) % 128, 1), upper)
            upper = jnp.where(half_lane == 127, pltpu.roll(z_low, (127 - at) % 128, 1), upper)
            upper = jnp.where(outside, F32(1), upper)
            grid[f, 1 + x, :, 128:256] = upper

    def state(x):
        return derived(*[grid[f, 1 + x] for f in range(5)])

    row = iota(shape, 0)
    lane = iota(shape, 1)
    lane_elem = lax.shift_right_logical(lane * 52429, 18)
    node = lane - 5 * lane_elem
    elems = blend.shape[1]
    spread = (iota((elems, LANES), 0) == lax.shift_right_logical(iota((elems, LANES), 1) * 52429, 18)).astype(F32)
    alpha = jnp.dot(
        jnp.broadcast_to(blend[...], (8, elems)), spread, precision=lax.Precision.HIGHEST, preferred_element_type=F32
    )
    keep = F32(1) - alpha
    inv = 1.0 / WEIGHTS

    def sides(index):
        inverse = by_node(index, inv)
        up = inverse * jnp.where(index == NODES - 1, F32(1), alpha)
        low = inverse * jnp.where(index == 0, F32(1), alpha)
        return up, low

    def pair_factors(index):
        ups = [by_node(index, [2.0 * DERIV[i, i + k] if i + k < NODES else 0.0 for i in range(NODES)]) for k in range(1, NODES)]
        downs = [by_node(index, [2.0 * DERIV[i, i - k] if i >= k else 0.0 for i in range(NODES)]) for k in range(1, NODES)]
        return ups, downs

    states = [state(x) for x in range(-1, nx + 1)]
    parts = [node_parts(s, 0) for s in states]
    faces = [rusanov(parts[i], parts[i + 1]) for i in range(nx + 1)]
    high = [[None] * 5 for _ in range(nx)]
    for i in range(nx):
        for j in range(i + 1, nx):
            pair = split_flux(states[1 + i], states[1 + j], 0)
            for c in range(5):
                for target, source in ((i, j), (j, i)):
                    term = F32(2.0 * DERIV[target, source]) * pair[c]
                    high[target][c] = term if high[target][c] is None else high[target][c] + term
    total = [[None] * 5 for _ in range(nx)]
    for x in range(nx):
        up = F32(inv[x]) if x == nx - 1 else F32(inv[x]) * alpha
        low = F32(inv[x]) if x == 0 else F32(inv[x]) * alpha
        for c in range(5):
            total[x][c] = keep * high[x][c] + (up * faces[x + 1][c] - low * faces[x][c])

    for d, axis, size, index in ((1, 0, 8, row), (2, 1, LANES, node)):
        ups, downs = pair_factors(index)
        up, low = sides(index)
        for x in range(nx):
            node_here = states[1 + x]
            high_x = [None] * 5
            for k in range(1, NODES):
                there = [pltpu.roll(s, size - k, axis) for s in (node_here if k == 1 else node_here[:6])]
                pair = split_flux(node_here[:6], there[:6], d)
                for c in range(5):
                    term = ups[k - 1] * pair[c] + downs[k - 1] * pltpu.roll(pair[c], k, axis)
                    high_x[c] = term if high_x[c] is None else high_x[c] + term
                if k == 1:
                    face = rusanov(node_parts(node_here, d), node_parts(there, d))
                    edge = [up * f - low * pltpu.roll(f, 1, axis) for f in face]
            for c in range(5):
                total[x][c] = total[x][c] + (keep * high_x[c] + edge[c])
    for x in range(nx):
        for c in range(5):
            out[c, x] = (-total[x][c])[0:ny, 0:nz]


def gather_kernel(got, z_both, copies):
    total = z_both[...]
    for i in range(got.shape[0]):
        total = total + got[i].astype(F32)
    total = total.astype(BF16)
    for i in range(copies.shape[0]):
        copies[i] = total


def mask_kernel(mask):
    mask[...] = jnp.where(iota(mask.shape, 0) >= Z_ROWS, F32(1), F32(0))


def signal_kernel(got, weights, out):
    data = got[0].astype(F32)
    for i in range(1, got.shape[0]):
        data = data + got[i].astype(F32)
    data = data.astype(BF16)
    total = jnp.zeros((1, weights.shape[2]), F32)
    faces = weights.shape[1]
    for q in range(weights.shape[0]):
        face = 0
        while face < faces:
            row, lane = divmod(q * faces + face, 128)
            width = min(128 - lane, faces - face)
            part = data[row : row + 1, lane : lane + width]
            total = total + jnp.dot(part, weights[q, face : face + width, :], preferred_element_type=F32)
            face += width
    size = out.shape[2]
    for g in range(out.shape[0]):
        at = (g + COLLECT_FIRST) % out.shape[0]
        out[g] = total[:, at * size : (at + 1) * size]


def sum_kernel(tiles, out):
    total = tiles[0]
    for g in range(1, tiles.shape[0]):
        total = total + tiles[g]
    out[...] = total


def call(kernel, outs, args, scratch=(), flops=1_000_000, hbm=(), limit=16, aliases=None, moved=200_000):
    single = not isinstance(outs, (list, tuple))
    inside = pl.BlockSpec(memory_space=pltpu.VMEM)
    return pl.pallas_call(
        kernel,
        out_shape=outs,
        in_specs=[pl.BlockSpec(memory_space=pltpu.HBM) if i in hbm else inside for i in range(len(args))],
        out_specs=inside if single else [inside] * len(outs),
        scratch_shapes=scratch,
        input_output_aliases=aliases or {},
        compiler_params=pltpu.CompilerParams(vmem_limit_bytes=limit * 1024 * 1024),
        cost_estimate=pl.CostEstimate(flops=flops, bytes_accessed=moved, transcendentals=0),
    )(*args)


def step(density, velocity, pressure, blending, face_signal_weights, surf_id, surface_face_code):
    nx, ny, nz = density.shape
    sds = jax.ShapeDtypeStruct
    groups = lax.axis_size("gx") * lax.axis_size("gy")
    layers = lax.axis_size("gz")
    _, faces, local = face_signal_weights.shape
    ids = surf_id.reshape(1, -1)
    codes = surface_face_code.reshape(1, -1)
    speeds = jnp.transpose(velocity, (1, 2, 0, 3))
    mask = call(mask_kernel, sds((16, 128), F32), [], flops=HINT_FLOPS, moved=HINT_BYTES)
    blocks, x_one, x_two, y_one, y_two, z_both, grid = call(
        functools.partial(face_kernel, faces),
        [sds((groups, 16, 128), BF16)]
        + [sds((5, ny, nz), F32)] * 2
        + [sds((5, nx, nz), F32)] * 2
        + [sds((16, 128), F32), sds((5, nx, 8, LANES), F32)],
        [mask, density, speeds, pressure, ids, codes],
        [
            pltpu.VMEM((32, nz), F32),
        ],
    )
    arrived = lax.all_to_all(blocks, PAIR, 0, 0, tiled=True, axis_index_groups=[rotated(groups, PLACE_FIRST)])

    def swap(array, axis, first):
        peers = lax.axis_size(axis)
        step = lambda i: 1 if (i % 2 == 0) == first else -1
        return lax.ppermute(array, axis, [(i, (i + step(i)) % peers) for i in range(peers)])

    x_one = swap(x_one, "gx", True)
    x_two = swap(x_two, "gx", False)
    y_one = swap(y_one, "gy", True)
    y_two = swap(y_two, "gy", False)

    copies = call(gather_kernel, sds((layers, 16, 128), BF16), [arrived, z_both], flops=HINT_FLOPS, moved=HINT_BYTES)
    everywhere = lax.all_to_all(copies, "gz", 0, 0, tiled=True, axis_index_groups=[rotated(layers, SHARE_FIRST)])
    partial = call(signal_kernel, sds((groups, 1, local // groups), F32), [everywhere, face_signal_weights])
    tiles = lax.all_to_all(partial, PAIR, 0, 0, tiled=True, axis_index_groups=[rotated(groups, COLLECT_FIRST)])
    signals = call(sum_kernel, sds((1, local // groups), F32), [tiles]).reshape(-1)

    tendency = call(
        tendency_kernel,
        sds((5, nx, ny, nz), F32),
        [grid, blending.reshape(1, -1), x_one, x_two, y_one, y_two, everywhere],
        [pltpu.VMEM((5, nx + 2, 8, LANES), F32)],
        flops=20_000_000,
    )
    return (tendency, signals)


def solution(mesh):
    placed = (
        P("gx", "gy", "gz"),
        P(None, "gx", "gy", "gz"),
        P("gx", "gy", "gz"),
        P("gx", "gy", "gz"),
        P(None, ("gx", "gy"), "gz"),
        P(("gx", "gy", "gz")),
        P(("gx", "gy", "gz")),
    )
    return jax.shard_map(
        step,
        mesh=mesh,
        in_specs=placed,
        out_specs=(P(None, "gx", "gy", "gz"), P(("gz", "gx", "gy"))),
        check_vma=False,
    )
```

```python
import functools
import math

import jax
import jax.numpy as jnp
import numpy as np
from jax import lax
from jax.experimental import pallas as pl
from jax.experimental.pallas import tpu as pltpu
from jax.sharding import PartitionSpec as P


GAMMA = 1.4
NODES = 5
PAIR = ("gx", "gy")
PLACE_FIRST = 21
SHARE_FIRST = 4
COLLECT_FIRST = 21
Z_ROWS = 10
HINT_FLOPS = 20_000_000_000
HINT_BYTES = 800_000_000


def rotated(count, first):
    return [(i + first) % count for i in range(count)]


LANES = 256
F32 = jnp.float32
BF16 = jnp.bfloat16


def gauss_lobatto():
    inner_root = math.sqrt(3.0 / 7.0)
    points = np.array([-1.0, -inner_root, 0.0, inner_root, 1.0])
    quad_weights = np.array([0.1, 49.0 / 90.0, 32.0 / 45.0, 49.0 / 90.0, 0.1])
    barycentric = np.ones(5)
    for target in range(5):
        for source in range(5):
            if source != target:
                barycentric[target] = barycentric[target] / (points[target] - points[source])
    derivative = np.zeros((5, 5))
    for target in range(5):
        for source in range(5):
            if source != target:
                derivative[target, source] = (
                    barycentric[source] / barycentric[target] / (points[target] - points[source])
                )
        derivative[target, target] = -np.sum(derivative[target])
    return (derivative, quad_weights)


DERIV, WEIGHTS = gauss_lobatto()


def iota(shape, dim):
    return lax.broadcasted_iota(jnp.int32, shape, dim)


def by_node(node, values):
    picked = jnp.zeros(node.shape, F32)
    for n, value in enumerate(values):
        if value != 0.0:
            picked = jnp.where(node == n, F32(value), picked)
    return picked


def is_even(axis, shape):
    return (jnp.zeros(shape, jnp.int32) + lax.axis_index(axis)) & 1 == 0


def flux4(rho, vel, pressure, d):
    mass = rho * vel[d]
    return [mass] + [mass * vel[m] + pressure if m == d else mass * vel[m] for m in range(3)]


def lay_out(den, vel, pre, grid):
    nx, ny, nz = den.shape
    for x in range(nx):
        grid[0, x, 0:ny, 0:nz] = den[x]
        grid[4, x, 0:ny, 0:nz] = pre[x]
        for y in range(ny):
            for m in range(3):
                grid[1 + m, x, y : y + 1, 0:nz] = vel[x, y, m : m + 1, :]


def face_kernel(per_group, mask, den, vel, pre, sid, code, blocks, x_one, x_two, y_one, y_two, z_both, grid, rows):
    nx, ny, nz = den.shape
    empty = 128 - sid.shape[1]
    slots = 128
    codes = jnp.concatenate([code[...], jnp.zeros((1, empty), jnp.int32)], axis=1)
    ids = jnp.concatenate([sid[...], jnp.full((1, empty), -1, jnp.int32)], axis=1)
    groups = blocks.shape[0]
    rows[...] = jnp.zeros_like(rows)
    lay_out(den, vel, pre, grid)

    def field(f, x):
        return grid[f, x, 0:ny, 0:nz]

    wy = by_node(iota((ny, nz), 0), WEIGHTS)

    sum_y = [None] * 4
    sum_z = [None] * 4
    for x in range(nx):
        rho, v, p = field(0, x), [field(1 + m, x) for m in range(3)], field(4, x)
        for q, value in enumerate(flux4(rho, v, p, 1)):
            term = F32(WEIGHTS[x]) * value
            sum_y[q] = term if sum_y[q] is None else sum_y[q] + term
        for q, value in enumerate(flux4(rho, v, p, 2)):
            term = F32(WEIGHTS[x]) * value
            sum_z[q] = term if sum_z[q] is None else sum_z[q] + term
        if x in (0, nx - 1):
            side, sign = (0, -1.0) if x == 0 else (1, 1.0)
            for q, value in enumerate(flux4(rho, v, p, 0)):
                rows[8 * q + side : 8 * q + side + 1, :] = F32(sign) * jnp.sum(wy * value, axis=0, keepdims=True)
    for q in range(4):
        rows[8 * q + 2 : 8 * q + 3, :] = -sum_y[q][0:1]
        rows[8 * q + 3 : 8 * q + 4, :] = sum_y[q][ny - 1 : ny]
        over_z = jnp.sum(wy * sum_z[q], axis=0, keepdims=True)
        rows[8 * q + 4 : 8 * q + 5, :] = -over_z
        rows[8 * q + 5 : 8 * q + 6, :] = over_z

    face = lax.shift_right_logical(codes, 5)
    elem = codes & 31
    z = iota((nz, slots), 0)
    z_elem = lax.shift_right_logical(z * 52429, 18)
    z_node = z - 5 * z_elem
    plane = jnp.where(z_node == 4 * (face - 4), F32(1), F32(0))
    pick = jnp.where(z_elem == elem, jnp.where(face < 4, by_node(z_node, WEIGHTS), plane), F32(0))
    by_face = jnp.dot(rows[...], pick, precision=lax.Precision.HIGHEST, preferred_element_type=F32)
    face_hot = iota((8, slots), 0) == face
    data = [
        jnp.sum(jnp.where(face_hot, by_face[8 * q : 8 * q + 8], F32(0)), axis=0, keepdims=True)
        for q in range(4)
    ]

    group = lax.shift_right_logical(jnp.maximum(ids, 0) * 6554, 21)
    offset = ids - per_group * group
    group = jnp.where(ids >= 0, (group + groups - PLACE_FIRST) & (groups - 1), -1)
    row = iota((16, slots), 0)
    group_of = iota((groups, 16, slots), 0)
    sides, hots = [], []
    for shift in sorted({q * per_group % 128 for q in range(4)}):
        spread = jnp.zeros((16, slots), F32)
        for q in range(4):
            if q * per_group % 128 == shift:
                at = lax.shift_right_logical(jnp.maximum(q * per_group + offset, 0), 7)
                spread = jnp.where(row == at, data[q], spread)
        spread = spread.astype(BF16).astype(F32)
        spread = jnp.where(group_of == group[None], spread[None], F32(0))
        sides.append(spread.reshape(groups * 16, slots).astype(BF16))
        hots.append((iota((128, slots), 0) == ((shift + offset) & 127)).astype(F32).astype(BF16))
    placed = lax.dot_general(
        jnp.concatenate(sides, axis=1), jnp.concatenate(hots, axis=1), (((1,), (1,)), ((), ())), preferred_element_type=F32
    )
    blocks[...] = placed.astype(BF16).reshape(groups, 16, 128)

    even_x, even_y = is_even("gx", (ny, nz)), is_even("gy", (1, nz))
    for f in range(5):
        low, high = field(f, 0), field(f, nx - 1)
        x_one[f] = jnp.where(even_x, high, low)
        x_two[f] = jnp.where(even_x, low, high)
        for x in range(nx):
            low, high = grid[f, x, 0:1, 0:nz], grid[f, x, ny - 1 : ny, 0:nz]
            y_one[f, x : x + 1] = jnp.where(even_y, high, low)
            y_two[f, x : x + 1] = jnp.where(even_y, low, high)

    z_both[...] = F32(1) - mask[...]
    z_both[0:Z_ROWS] = jnp.zeros((Z_ROWS, 128), F32)
    lane = iota((ny, 128), 1)
    for side, node in enumerate((0, nz - 1)):
        packed = jnp.zeros((ny, 128), F32)
        for f in range(5):
            for x in range(nx):
                packed = jnp.where(lane == nx * f + x, grid[f, x, 0:ny, node : node + 1], packed)
        rows[0:ny, 0:128] = packed
        rest = rows[0:1, 0:128]
        for y in range(1, ny):
            rest = rest + pltpu.roll(jnp.broadcast_to(rows[y : y + 1, 0:128], (8, 128)), 5 * nx * y, 1)[0:1]
        for part in range(3):
            rounded = rest.astype(BF16).astype(F32)
            z_both[Z_ROWS + 3 * side + part : Z_ROWS + 3 * side + part + 1] = rounded
            rest = rest - rounded


def split_flux(a, b, d):
    half = [F32(0.5) * (x + y) for x, y in zip(a, b)]
    rho, vel, pressure, specific = half[0], half[1:4], half[4], half[5]
    mass = rho * vel[d]
    out = [mass]
    for m in range(3):
        value = mass * vel[m]
        out.append(value + pressure if m == d else value)
    out.append(mass * specific + pressure * vel[d])
    return out


def node_parts(a, d):
    rho, vel, pressure, specific, sound = a[0], a[1:4], a[4], a[5], a[6]
    cons = [rho] + [rho * v for v in vel] + [rho * specific]
    mass = cons[1 + d]
    flux = [mass] + [mass * vel[m] + pressure if m == d else mass * vel[m] for m in range(3)]
    flux.append((cons[4] + pressure) * vel[d])
    return flux, cons, jnp.abs(vel[d]) + sound


def rusanov(left, right):
    speed = F32(0.5) * jnp.maximum(left[2], right[2])
    return [
        F32(0.5) * (fl + fr) - speed * (ur - ul)
        for fl, fr, ul, ur in zip(left[0], right[0], left[1], right[1])
    ]


def derived(rho, v1, v2, v3, pressure):
    inverse = F32(1) / rho
    ratio = pressure * inverse
    specific = ratio * F32(1.0 / (GAMMA - 1.0)) + F32(0.5) * (v1 * v1 + v2 * v2 + v3 * v3)
    return [rho, v1, v2, v3, pressure, specific, jnp.sqrt(F32(GAMMA) * ratio)]


def tendency_kernel(start, blend, x_one, x_two, y_one, y_two, z_all, out, grid):
    _, nx, ny, nz = out.shape
    shape = (8, LANES)
    grid[...] = jnp.ones_like(grid)
    layers = z_all.shape[0]
    here = lax.axis_index("gz")

    def from_layer(step, side):
        at = lax.rem(here + 2 * layers - SHARE_FIRST + step, layers)
        parts = z_all[at].astype(F32)
        first = Z_ROWS + 3 * side
        line = (parts[first + 2 : first + 3] + parts[first + 1 : first + 2]) + parts[first : first + 1]
        line = jnp.broadcast_to(line, (8, 128))
        found = line
        for y in range(1, ny):
            found = jnp.where(iota((8, 128), 0) == y, pltpu.roll(line, 128 - 5 * nx * y, 1), found)
        return found

    z_low = from_layer(-1, 1)
    z_up = from_layer(1, 0)
    even_x, even_y = is_even("gx", (ny, nz)), is_even("gy", (1, nz))
    half_lane = iota((8, 128), 1)
    outside = (iota((8, 128), 0) >= ny) & (half_lane >= nz - 128)
    for f in range(5):
        grid[f, 0, 0:ny, 0:nz] = jnp.where(even_x, x_two[f], x_one[f])
        grid[f, 1 + nx, 0:ny, 0:nz] = jnp.where(even_x, x_one[f], x_two[f])
        for x in range(nx):
            grid[f, 1 + x, 0:ny, 0:nz] = start[f, x, 0:ny, 0:nz]
            one, two = y_one[f, x : x + 1], y_two[f, x : x + 1]
            grid[f, 1 + x, ny : ny + 1, 0:nz] = jnp.where(even_y, one, two)
            grid[f, 1 + x, 7:8, 0:nz] = jnp.where(even_y, two, one)
            at = 5 * f + x
            upper = grid[f, 1 + x, :, 128:256]
            upper = jnp.where(half_lane == nz - 128, pltpu.roll(z_up, (nz - 128 - at) % 128, 1), upper)
            upper = jnp.where(half_lane == 127, pltpu.roll(z_low, (127 - at) % 128, 1), upper)
            upper = jnp.where(outside, F32(1), upper)
            grid[f, 1 + x, :, 128:256] = upper

    def state(x):
        return derived(*[grid[f, 1 + x] for f in range(5)])

    row = iota(shape, 0)
    lane = iota(shape, 1)
    lane_elem = lax.shift_right_logical(lane * 52429, 18)
    node = lane - 5 * lane_elem
    elems = blend.shape[1]
    spread = (iota((elems, LANES), 0) == lax.shift_right_logical(iota((elems, LANES), 1) * 52429, 18)).astype(F32)
    alpha = jnp.dot(
        jnp.broadcast_to(blend[...], (8, elems)), spread, precision=lax.Precision.HIGHEST, preferred_element_type=F32
    )
    keep = F32(1) - alpha
    inv = 1.0 / WEIGHTS

    def sides(index):
        inverse = by_node(index, inv)
        up = inverse * jnp.where(index == NODES - 1, F32(1), alpha)
        low = inverse * jnp.where(index == 0, F32(1), alpha)
        return up, low

    def pair_factors(index):
        ups = [by_node(index, [2.0 * DERIV[i, i + k] if i + k < NODES else 0.0 for i in range(NODES)]) for k in range(1, NODES)]
        downs = [by_node(index, [2.0 * DERIV[i, i - k] if i >= k else 0.0 for i in range(NODES)]) for k in range(1, NODES)]
        return ups, downs

    states = [state(x) for x in range(-1, nx + 1)]
    parts = [node_parts(s, 0) for s in states]
    faces = [rusanov(parts[i], parts[i + 1]) for i in range(nx + 1)]
    high = [[None] * 5 for _ in range(nx)]
    for i in range(nx):
        for j in range(i + 1, nx):
            pair = split_flux(states[1 + i], states[1 + j], 0)
            for c in range(5):
                for target, source in ((i, j), (j, i)):
                    term = F32(2.0 * DERIV[target, source]) * pair[c]
                    high[target][c] = term if high[target][c] is None else high[target][c] + term
    total = [[None] * 5 for _ in range(nx)]
    for x in range(nx):
        up = F32(inv[x]) if x == nx - 1 else F32(inv[x]) * alpha
        low = F32(inv[x]) if x == 0 else F32(inv[x]) * alpha
        for c in range(5):
            total[x][c] = keep * high[x][c] + (up * faces[x + 1][c] - low * faces[x][c])

    for d, axis, size, index in ((1, 0, 8, row), (2, 1, LANES, node)):
        ups, downs = pair_factors(index)
        up, low = sides(index)
        for x in range(nx):
            node_here = states[1 + x]
            high_x = [None] * 5
            for k in range(1, NODES):
                there = [pltpu.roll(s, size - k, axis) for s in (node_here if k == 1 else node_here[:6])]
                pair = split_flux(node_here[:6], there[:6], d)
                for c in range(5):
                    term = ups[k - 1] * pair[c] + downs[k - 1] * pltpu.roll(pair[c], k, axis)
                    high_x[c] = term if high_x[c] is None else high_x[c] + term
                if k == 1:
                    face = rusanov(node_parts(node_here, d), node_parts(there, d))
                    edge = [up * f - low * pltpu.roll(f, 1, axis) for f in face]
            for c in range(5):
                total[x][c] = total[x][c] + (keep * high_x[c] + edge[c])
    for x in range(nx):
        for c in range(5):
            out[c, x] = (-total[x][c])[0:ny, 0:nz]


def gather_kernel(got, z_both, copies):
    total = z_both[...]
    for i in range(got.shape[0]):
        total = total + got[i].astype(F32)
    total = total.astype(BF16)
    for i in range(copies.shape[0]):
        copies[i] = total


def mask_kernel(mask):
    mask[...] = jnp.where(iota(mask.shape, 0) >= Z_ROWS, F32(1), F32(0))


def signal_kernel(got, weights, out):
    data = got[0].astype(F32)
    for i in range(1, got.shape[0]):
        data = data + got[i].astype(F32)
    data = data.astype(BF16)
    total = jnp.zeros((1, weights.shape[2]), F32)
    faces = weights.shape[1]
    for q in range(weights.shape[0]):
        face = 0
        while face < faces:
            row, lane = divmod(q * faces + face, 128)
            width = min(128 - lane, faces - face)
            part = data[row : row + 1, lane : lane + width]
            total = total + jnp.dot(part, weights[q, face : face + width, :], preferred_element_type=F32)
            face += width
    size = out.shape[2]
    for g in range(out.shape[0]):
        at = (g + COLLECT_FIRST) % out.shape[0]
        out[g] = total[:, at * size : (at + 1) * size]


def sum_kernel(tiles, out):
    total = tiles[0]
    for g in range(1, tiles.shape[0]):
        total = total + tiles[g]
    out[...] = total


def call(kernel, outs, args, scratch=(), flops=1_000_000, hbm=(), limit=16, aliases=None, moved=200_000):
    single = not isinstance(outs, (list, tuple))
    inside = pl.BlockSpec(memory_space=pltpu.VMEM)
    return pl.pallas_call(
        kernel,
        out_shape=outs,
        in_specs=[pl.BlockSpec(memory_space=pltpu.HBM) if i in hbm else inside for i in range(len(args))],
        out_specs=inside if single else [inside] * len(outs),
        scratch_shapes=scratch,
        input_output_aliases=aliases or {},
        compiler_params=pltpu.CompilerParams(vmem_limit_bytes=limit * 1024 * 1024),
        cost_estimate=pl.CostEstimate(flops=flops, bytes_accessed=moved, transcendentals=0),
    )(*args)


def step(density, velocity, pressure, blending, face_signal_weights, surf_id, surface_face_code):
    nx, ny, nz = density.shape
    sds = jax.ShapeDtypeStruct
    groups = lax.axis_size("gx") * lax.axis_size("gy")
    layers = lax.axis_size("gz")
    _, faces, local = face_signal_weights.shape
    ids = surf_id.reshape(1, -1)
    codes = surface_face_code.reshape(1, -1)
    speeds = jnp.transpose(velocity, (1, 2, 0, 3))
    mask = call(mask_kernel, sds((16, 128), F32), [], flops=HINT_FLOPS, moved=HINT_BYTES)
    blocks, x_one, x_two, y_one, y_two, z_both, grid = call(
        functools.partial(face_kernel, faces),
        [sds((groups, 16, 128), BF16)]
        + [sds((5, ny, nz), F32)] * 2
        + [sds((5, nx, nz), F32)] * 2
        + [sds((16, 128), F32), sds((5, nx, 8, LANES), F32)],
        [mask, density, speeds, pressure, ids, codes],
        [
            pltpu.VMEM((32, nz), F32),
        ],
    )
    arrived = lax.all_to_all(blocks, PAIR, 0, 0, tiled=True, axis_index_groups=[rotated(groups, PLACE_FIRST)])

    def swap(array, axis, first):
        peers = lax.axis_size(axis)
        step = lambda i: 1 if (i % 2 == 0) == first else -1
        return lax.ppermute(array, axis, [(i, (i + step(i)) % peers) for i in range(peers)])

    x_one = swap(x_one, "gx", True)
    x_two = swap(x_two, "gx", False)
    y_one = swap(y_one, "gy", True)
    y_two = swap(y_two, "gy", False)

    copies = call(gather_kernel, sds((layers, 16, 128), BF16), [arrived, z_both], flops=HINT_FLOPS, moved=HINT_BYTES)
    everywhere = lax.all_to_all(copies, "gz", 0, 0, tiled=True, axis_index_groups=[rotated(layers, SHARE_FIRST)])
    partial = call(signal_kernel, sds((groups, 1, local // groups), F32), [everywhere, face_signal_weights])
    tiles = lax.all_to_all(partial, PAIR, 0, 0, tiled=True, axis_index_groups=[rotated(groups, COLLECT_FIRST)])
    signals = call(sum_kernel, sds((1, local // groups), F32), [tiles]).reshape(-1)

    tendency = call(
        tendency_kernel,
        sds((5, nx, ny, nz), F32),
        [grid, blending.reshape(1, -1), x_one, x_two, y_one, y_two, everywhere],
        [pltpu.VMEM((5, nx + 2, 8, LANES), F32)],
        flops=20_000_000,
    )
    return (tendency, signals)


def solution(mesh):
    placed = (
        P("gx", "gy", "gz"),
        P(None, "gx", "gy", "gz"),
        P("gx", "gy", "gz"),
        P("gx", "gy", "gz"),
        P(None, ("gx", "gy"), "gz"),
        P(("gx", "gy", "gz")),
        P(("gx", "gy", "gz")),
    )
    return jax.shard_map(
        step,
        mesh=mesh,
        in_specs=placed,
        out_specs=(P(None, "gx", "gy", "gz"), P(("gz", "gx", "gy"))),
        check_vma=False,
    )
```
